32 devices in a mesh: section: 16 (over z, y, core), walk: 2 (over x).
Axes of the slice: x: 2, y: 2, z: 4, core: 2. Of those that a mesh axis runs over, the one named last changes fastest.
Arguments:
- fields: bfloat16 [16, 8, 800], P('section', None, 'walk'), may hold values from -4 to 4
- cholesky_vectors: bfloat16 [800, 200, 200], P('walk'), may hold values from -0.013 to 0.013
- trial_state: float32 [200, 100], replicated, may hold values from -1.6 to 1.6
- deviation: bfloat16 [16, 8, 200, 100], P('section', 'walk'), may hold values from -0.1796875 to 0.1796875
Outputs:
- density: float32 [8, 200, 200], P('walk')
The draws below stay inside these ranges and needn't reach their ends.
All inputs are finite; a program needn't handle non-finite values.
Results may differ from the reference program's by a relative error of at most 0.0003.
Values sent between devices are 32-bit elements; how exact they have to be, the bound alone decides.
A program may use at most 128 MiB of HBM per device.

```python
import jax
import jax.numpy as jnp
from jax import lax

ORB = 200
ELEC = 100
CHOL = 800
TAYLOR = 6
STEPS = 16
WALKERS = 8


def draw_trial_state(key, part):
    diag_key = jax.random.fold_in(key, 11)
    upper_key = jax.random.fold_in(key, 12)
    lower_key = jax.random.fold_in(key, 13)
    diagonal_part = jax.random.uniform(diag_key, (ELEC,), jnp.float32, 0.8, 1.2)
    upper_noise = 0.3 * jax.random.normal(upper_key, (ELEC, ELEC), jnp.float32) / ELEC ** 0.5
    lower_noise = 0.3 * jax.random.normal(lower_key, (ORB - ELEC, ELEC), jnp.float32) / ORB ** 0.5
    upper_block = jnp.diag(diagonal_part) + upper_noise
    return jnp.clip(jnp.concatenate([upper_block, lower_noise], axis=0), -1.6, 1.6)


def draw_cholesky_vectors(key, part):
    base_key = jax.random.fold_in(key, 21)
    raw_draw = jnp.clip(jax.random.normal(base_key, (CHOL, ORB, ORB), jnp.float32), -4.0, 4.0)
    upper_part = jnp.triu(raw_draw, 1)
    generator = upper_part - jnp.swapaxes(upper_part, 1, 2)
    positions = jnp.arange(ORB)
    occupied = positions < ELEC
    same_block = occupied[:, None] == occupied[None, :]
    inside_scale = 1.8 / (2.0 * ORB * CHOL) ** 0.5
    across_scale = 0.6 / (2.0 * ORB * CHOL * STEPS) ** 0.5
    entry_scale = jnp.where(same_block, inside_scale, across_scale)
    return (generator * entry_scale).astype(jnp.bfloat16)


def block_scale(key, dims, cuts, least, high):
    level, own = 1.0, jax.random.fold_in(key, 6)
    for position, blocks in cuts:
        draws = jnp.exp(jax.random.uniform(jax.random.fold_in(own, position), (blocks,), jnp.float32, least / len(cuts), high / len(cuts)))
        level = level * jnp.repeat(draws, dims[position] // blocks).reshape([-1 if axis == position else 1 for axis in range(len(dims))])
    return level


def normal_values(rng, dims, scale, bound, pieces=(), dtype=jnp.bfloat16):
    values = scale * jax.random.normal(rng, dims, jnp.float32)
    if pieces:
        values = values * block_scale(rng, dims, pieces, -0.22, 0.18)
    return jnp.clip(values, -bound, bound).astype(dtype)


def setup_inputs(seed: int = 0) -> dict:
    keys = jax.random.split(jax.random.key(seed), 5)
    fields = normal_values(keys[0], (STEPS, WALKERS, CHOL), 1.0, 4.0, ((0, 16), (2, 2)))
    cholesky_vectors = draw_cholesky_vectors(jax.random.fold_in(keys[4], 71), 0)
    trial_state = draw_trial_state(jax.random.fold_in(keys[4], 71), 0)
    deviation = normal_values(keys[3], (STEPS, WALKERS, ORB, ELEC), 0.03, 0.1796875, ((0, 16), (1, 2)))
    return dict(fields=fields, cholesky_vectors=cholesky_vectors, trial_state=trial_state, deviation=deviation)


exact_mode = lax.Precision.HIGHEST

def apply_series(field_matrix, left_state):
    series_term = left_state
    summed = left_state
    for degree in range(1, TAYLOR + 1):
        series_term = jnp.einsum('wij,wie->wje', field_matrix, series_term, precision=exact_mode) / degree
        summed = summed + series_term
    return summed

def green_block(left_state, walker):
    intersection = jnp.einsum('wie,wif->wef', left_state, walker, precision=exact_mode)
    solved = jnp.linalg.solve(intersection, jnp.swapaxes(left_state, 1, 2))
    return jnp.einsum('wie,wej->wij', walker, solved, precision=exact_mode)

def reference(fields, cholesky_vectors, trial_state, deviation):
    vector_table = cholesky_vectors.reshape(CHOL, ORB * ORB)
    start_left = jnp.broadcast_to(trial_state, (WALKERS, ORB, ELEC)).astype(jnp.float32)

    def step(state_pair, step_inputs):
        left_state, running = state_pair
        field_row, deviation_row = step_inputs
        field_matrix = jnp.dot(field_row.astype(jnp.float32), vector_table.astype(jnp.float32), preferred_element_type=jnp.float32).reshape(WALKERS, ORB, ORB)
        left_state = apply_series(field_matrix, left_state)
        walker = trial_state + deviation_row.astype(jnp.float32)
        running = running + green_block(left_state, walker)
        return ((left_state, running), None)
    initial = (start_left, jnp.zeros((WALKERS, ORB, ORB), jnp.float32))
    (left_state, running), _ = lax.scan(step, initial, (fields, deviation), reverse=True)
    return running / STEPS
```

```python
import functools

import jax
import jax.numpy as jnp
from jax import lax
from jax.experimental import pallas as pl
from jax.experimental.pallas import tpu as pltpu
from jax.sharding import Mesh, PartitionSpec as P


SUB = 8
LANES = 128
DEPTH = 4
LAG = 4
MESH = pl.DeviceIdType.MESH


def split(a):
    high = a.astype(jnp.bfloat16)
    return high, (a - high.astype(jnp.float32)).astype(jnp.bfloat16)


def dot_f32(a, b):
    return jnp.dot(a, b, preferred_element_type=jnp.float32)


def dot3(a, b):
    a_high, a_low = split(a)
    b_high, b_low = split(b)
    return dot_f32(a_high, b_high) + (dot_f32(a_high, b_low) + dot_f32(a_low, b_high))


def greet(peers):
    barrier = pltpu.get_barrier_semaphore()
    for axis, peer in peers:
        pl.semaphore_signal(barrier, inc=1, device_id={axis: peer}, device_id_type=MESH)
    return barrier


def fold_rows(orbitals):
    return (orbitals // SUB + 1) // 2 * SUB


def contract_kernel(
    field_ref, table_ref, trial_ref, deviation_ref, packed_ref, walkers_ref,
    factor, low, high, part, arrived, total, gathered, walk_send, walk_recv,
    low_sem, high_sem, x_send, x_recv, m_send, m_recv, w_send, w_recv,
):
    rows, chol = field_ref.shape
    per, orbitals, electrons = deviation_ref.shape
    members, walks = lax.axis_size("member"), lax.axis_size("walk")
    member, walk = lax.axis_index("member"), lax.axis_index("walk")
    half = fold_rows(orbitals)
    bands, folds = orbitals // SUB, half // SUB
    depth = chol * SUB
    order = [band for f in range(folds) for band in (f, f + folds) if band < bands]

    def fetch(place):
        band, slot = order[place], place % DEPTH
        at = pl.ds(band * SUB, SUB)
        copies = [
            pltpu.make_async_copy(
                table_ref.at[:, at, pl.ds(LANES, orbitals - LANES)], high.at[slot], high_sem.at[slot]
            )
        ]
        if band * SUB < LANES:
            copies.append(
                pltpu.make_async_copy(
                    table_ref.at[:, at, pl.ds(0, LANES)], low.at[slot], low_sem.at[slot]
                )
            )
        return copies

    flight = {}

    def start(place):
        if place < len(order):
            flight[place] = fetch(place)
            for copy in flight[place]:
                copy.start()

    for place in range(DEPTH):
        start(place)
    barrier = greet(
        [("walk", lax.rem(walk + s, walks)) for s in range(1, walks)]
        + [("member", lax.rem(member + s, members)) for s in range(1, members)]
    )
    walk_send[...] = trial_ref[...] + deviation_ref[...].astype(jnp.float32)

    vector = lax.broadcasted_iota(jnp.int32, (chol, LANES), 0)
    lane = lax.broadcasted_iota(jnp.int32, (chol, LANES), 1)
    keep = lax.broadcasted_iota(jnp.int32, (2 * SUB, LANES), 0) % SUB
    keep = keep == lax.broadcasted_iota(jnp.int32, (2 * SUB, LANES), 1) % SUB
    for j in range(pl.cdiv(depth, LANES)):
        width = min(LANES, depth - j * LANES)
        pick = jnp.where(vector == j * (LANES // SUB) + lane // SUB, 1.0, 0.0)
        spread = dot_f32(field_ref[...], pick.astype(jnp.bfloat16))
        for row in range(0, rows, 2):
            pair = jnp.concatenate(
                [
                    jnp.broadcast_to(spread[row + i : row + i + 1], (SUB, LANES))
                    for i in range(2)
                ],
                axis=0,
            )
            factor[row * SUB : (row + 2) * SUB, j * LANES : j * LANES + width] = jnp.where(
                keep, pair, 0.0
            ).astype(jnp.bfloat16)[:, :width]

    def product(place):
        band, slot = order[place], place % DEPTH
        for copy in flight[place]:
            copy.wait()
        right = dot_f32(factor[...], high[slot].reshape(depth, orbitals - LANES))
        right = right.reshape(rows, SUB, orbitals - LANES)
        left = None
        if band * SUB < LANES:
            left = dot_f32(factor[...], low[slot].reshape(depth, LANES))
            left = left.reshape(rows, SUB, LANES)
        return left, right

    def x_copy(shift, f):
        peer = lax.rem(walk + shift, walks)
        at = pl.ds(f * SUB, SUB)
        return pltpu.make_async_remote_copy(
            src_ref=part.at[pl.ds(peer * per, per), at, :],
            dst_ref=arrived.at[shift - 1, :, at, :],
            send_sem=x_send.at[shift - 1, f],
            recv_sem=x_recv.at[shift - 1, f],
            device_id={"walk": peer},
            device_id_type=MESH,
        )

    def m_copy(shift, f):
        peer = lax.rem(member + shift, members)
        at = pl.ds(f * SUB, SUB)
        return pltpu.make_async_remote_copy(
            src_ref=total.at[peer, at, :],
            dst_ref=gathered.at[member, at, :],
            send_sem=m_send.at[shift - 1, f],
            recv_sem=m_recv.at[shift - 1, f],
            device_id={"member": peer},
            device_id_type=MESH,
        )

    def w_copy(shift):
        peer = lax.rem(member + shift, members)
        return pltpu.make_async_remote_copy(
            src_ref=walk_send.at[peer],
            dst_ref=walk_recv.at[member],
            send_sem=w_send.at[shift - 1],
            recv_sem=w_recv.at[shift - 1],
            device_id={"member": peer},
            device_id_type=MESH,
        )

    def merge(f):
        at = slice(f * SUB, (f + 1) * SUB)
        value = part[pl.ds(walk * per, per), at, :]
        for shift in range(1, walks):
            x_copy(shift, f).wait_recv()
            value = value + arrived[shift - 1, :, at, :]
        total[:, at, :] = value

    sub = lax.broadcasted_iota(jnp.int32, (SUB, orbitals), 0)
    column = lax.broadcasted_iota(jnp.int32, (SUB, orbitals), 1)
    place = 0
    for f in range(folds + LAG + 1):
        if f < folds:
            left, right = product(place)
            start(place + DEPTH)
            place += 1
            upper = jnp.concatenate([left, right], axis=2)
            if f + folds < bands:
                left, right = product(place)
                start(place + DEPTH)
                place += 1
                if left is not None:
                    right = jnp.concatenate([left[:, :, half:], right], axis=2)
                    pad = 0
                else:
                    pad = LANES - half
                pieces = [right, jnp.zeros((rows, SUB, half), jnp.float32)]
                if pad:
                    pieces = [jnp.zeros((rows, SUB, pad), jnp.float32)] + pieces
                lower = jnp.concatenate(pieces, axis=2)
            else:
                lower = jnp.zeros_like(upper)
            own = (column >= half) | (column < f * SUB + sub)
            part[:, f * SUB : (f + 1) * SUB, :] = jnp.where(own[None], upper, lower)
        if f == 0:
            pl.semaphore_wait(barrier, walks + members - 2)
            for shift in range(1, members):
                w_copy(shift).start()
        if 1 <= f <= folds:
            for shift in range(1, walks):
                x_copy(shift, f - 1).start()
        if f > LAG:
            for shift in range(1, members):
                m_copy(shift, f - LAG - 1).start()
        if f >= LAG and f - LAG < folds:
            merge(f - LAG)
    packed_ref[member] = total[member]
    walkers_ref[member] = walk_send[member]
    for shift in range(1, members):
        source = lax.rem(member + members - shift, members)
        w_copy(shift).wait()
        walkers_ref[source] = walk_recv[source]
        for f in range(folds):
            m_copy(shift, f).wait()
        packed_ref[source] = gathered[source]
    for shift in range(1, walks):
        for f in range(folds):
            x_copy(shift, f).wait_send()


def contract(field_rows, cholesky_vectors, trial_state, deviation):
    rows, chol = field_rows.shape
    per, orbitals, electrons = deviation.shape
    members, walks = lax.axis_size("member"), lax.axis_size("walk")
    half = fold_rows(orbitals)
    folds = half // SUB
    vmem = pl.BlockSpec(memory_space=pltpu.VMEM)
    f32, bf16, dma = jnp.float32, jnp.bfloat16, pltpu.SemaphoreType.DMA
    return pl.pallas_call(
        contract_kernel,
        in_specs=[vmem, pl.BlockSpec(memory_space=pl.ANY), vmem, vmem],
        out_specs=[vmem, vmem],
        out_shape=[
            jax.ShapeDtypeStruct((members, half, orbitals), f32),
            jax.ShapeDtypeStruct((members, orbitals, electrons), f32),
        ],
        scratch_shapes=[
            pltpu.VMEM((rows * SUB, chol * SUB), bf16),
            pltpu.VMEM((DEPTH, chol, SUB, LANES), bf16),
            pltpu.VMEM((DEPTH, chol, SUB, orbitals - LANES), bf16),
            pltpu.VMEM((rows, half, orbitals), f32),
            pltpu.VMEM((walks - 1, per, half, orbitals), f32),
            pltpu.VMEM((per, half, orbitals), f32),
            pltpu.VMEM((members, half, orbitals), f32),
            pltpu.VMEM((per, orbitals, electrons), f32),
            pltpu.VMEM((members, orbitals, electrons), f32),
            dma((DEPTH,)),
            dma((DEPTH,)),
            dma((walks - 1, folds)),
            dma((walks - 1, folds)),
            dma((members - 1, folds)),
            dma((members - 1, folds)),
            dma((members - 1,)),
            dma((members - 1,)),
        ],
        compiler_params=pltpu.CompilerParams(
            vmem_limit_bytes=48 * 2**20, collective_id=0, has_side_effects=True
        ),
    )(field_rows, cholesky_vectors, trial_state, deviation)


def eye(size):
    row = lax.broadcasted_iota(jnp.int32, (size, size), 0)
    column = lax.broadcasted_iota(jnp.int32, (size, size), 1)
    return jnp.where(row == column, 1.0, 0.0)


def unfold(packed):
    half, orbitals = packed.shape
    rest = orbitals - half
    row = lax.broadcasted_iota(jnp.int32, (half, half), 0)
    column = lax.broadcasted_iota(jnp.int32, (half, half), 1)
    square = packed[:, :half]
    flipped = -square.T
    first = jnp.where(row > column, square, jnp.where(row < column, flipped, 0.0))
    second = jnp.where(row < column, square, jnp.where(row > column, flipped, 0.0))
    across = packed[:, half:]
    return jnp.concatenate(
        [
            jnp.concatenate([first, across], axis=1),
            jnp.concatenate([-across.T, second[:rest, :rest]], axis=1),
        ],
        axis=0,
    )


def series(v, unit):
    v2 = dot3(v, v)
    v3 = dot3(v2, v)
    upper = unit * (1 / 6) + v * (1 / 24) + v2 * (1 / 120) + v3 * (1 / 720)
    return (unit + v + v2 * 0.5) + dot3(v3, upper)


def chain_kernel(packed_ref, trial_ref, steps_ref, left_ref, held, sent, send_sem, recv_sem):
    members = packed_ref.shape[0]
    padded, orbitals = held.shape
    blocks, block = lax.axis_size("block"), lax.axis_index("block")
    has_next, has_last = block < blocks - 1, block > 0
    cuts = [0, (padded // SUB + 1) // 2 * SUB, padded]
    barrier = pltpu.get_barrier_semaphore()
    for near, step in ((has_next, 1), (has_last, -1)):
        @pl.when(near)
        def _():
            pl.semaphore_signal(
                barrier, inc=1, device_id={"block": block + step}, device_id_type=MESH
            )

    unit = eye(orbitals)
    for s in range(members):
        steps_ref[s] = series(unfold(packed_ref[s]), unit)
    parts = [steps_ref[s] for s in reversed(range(members))]
    while len(parts) > 1:
        paired = [dot3(parts[i], parts[i + 1]) for i in range(0, len(parts) - 1, 2)]
        parts = paired + parts[len(parts) - len(parts) % 2 :]
    step_map = parts[0]
    pl.semaphore_wait(barrier, has_next.astype(jnp.int32) + has_last.astype(jnp.int32))

    def copy(i):
        at = pl.ds(cuts[i], cuts[i + 1] - cuts[i])
        return pltpu.make_async_remote_copy(
            src_ref=sent.at[at, :],
            dst_ref=held.at[at, :],
            send_sem=send_sem.at[i],
            recv_sem=recv_sem.at[i],
            device_id={"block": lax.rem(block + blocks - 1, blocks)},
            device_id_type=MESH,
        )

    @pl.when(jnp.logical_not(has_next))
    def _():
        held[...] = trial_ref[...]

    for i in range(len(cuts) - 1):
        @pl.when(has_next)
        def _():
            copy(i).wait_recv()

        @pl.when(has_last)
        def _():
            at = slice(cuts[i], cuts[i + 1])
            sent[at, :] = dot3(held[at, :], step_map)
            copy(i).start()

    left_ref[...] = held[: left_ref.shape[0], :]

    @pl.when(has_last)
    def _():
        for i in range(len(cuts) - 1):
            copy(i).wait_send()


def chain(packed, trial_state):
    members = packed.shape[0]
    orbitals, electrons = trial_state.shape
    padded = -(-electrons // SUB) * SUB
    trial = jnp.pad(trial_state.T, ((0, padded - electrons), (0, 0)))
    vmem = pl.BlockSpec(memory_space=pltpu.VMEM)
    return pl.pallas_call(
        chain_kernel,
        in_specs=[vmem, vmem],
        out_specs=[vmem, vmem],
        out_shape=[
            jax.ShapeDtypeStruct((members, orbitals, orbitals), jnp.float32),
            jax.ShapeDtypeStruct((electrons, orbitals), jnp.float32),
        ],
        scratch_shapes=[
            pltpu.VMEM((padded, orbitals), jnp.float32),
            pltpu.VMEM((padded, orbitals), jnp.float32),
            pltpu.SemaphoreType.DMA((2,)),
            pltpu.SemaphoreType.DMA((2,)),
        ],
        compiler_params=pltpu.CompilerParams(
            vmem_limit_bytes=48 * 2**20, collective_id=1, has_side_effects=True
        ),
    )(packed, trial)


def green_kernel(
    scale, left_in_ref, steps_ref, walk_ref, out_ref, left_ref, inter_ref, inverse_ref
):
    members = steps_ref.shape[0]
    unit = eye(left_in_ref.shape[0])
    left = left_in_ref[...]
    for s in reversed(range(members)):
        left = dot3(left, steps_ref[s])
        left_ref[s] = left
    for s in range(members):
        inter = dot3(left_ref[s], walk_ref[s])
        inter_ref[s] = inter
        flipped = inter.T
        square = dot3(inter, flipped)
        inverse_ref[s] = flipped * lax.rsqrt(jnp.sum(square * square))

    def newton():
        worst = jnp.float32(0.0)
        for s in range(members):
            guess = inverse_ref[s]
            rest = unit - dot3(inter_ref[s], guess)
            inverse_ref[s] = guess + dot3(guess, rest)
            worst = jnp.maximum(worst, jnp.sum(rest * rest))
        return worst

    def going(state):
        return (state[0] < 80) & (state[1] > 1e-4)

    lax.while_loop(going, lambda state: (state[0] + 1, newton()), (jnp.int32(0), jnp.float32(1.0)))
    newton()
    total = None
    for s in range(members):
        green = dot3(walk_ref[s], dot3(inverse_ref[s], left_ref[s]))
        total = green if total is None else total + green
    out_ref[...] = total * scale


def call(kernel, out_shape, args, scratch=(), scalars=0):
    vmem = pl.BlockSpec(memory_space=pltpu.VMEM)
    smem = pl.BlockSpec(memory_space=pltpu.SMEM)
    return pl.pallas_call(
        kernel,
        in_specs=[smem] * scalars + [vmem] * (len(args) - scalars),
        out_specs=vmem,
        out_shape=out_shape,
        scratch_shapes=list(scratch),
        compiler_params=pltpu.CompilerParams(vmem_limit_bytes=48 * 2**20),
    )(*args)


def total_over(array, axis):
    size = lax.axis_size(axis)
    if size & (size - 1):
        return lax.psum(array, axis)
    distance = 1
    while distance < size:
        array = array + lax.ppermute(array, axis, [(i, i ^ distance) for i in range(size)])
        distance *= 2
    return array


def body(fields, cholesky_vectors, trial_state, deviation):
    chol = fields.shape[2]
    orbitals, electrons = trial_state.shape
    blocks, members = lax.axis_size("block"), lax.axis_size("member")
    packed, walkers = contract(
        fields.reshape(-1, chol), cholesky_vectors, trial_state, deviation[0]
    )
    steps, left = chain(packed, trial_state)
    square = jax.ShapeDtypeStruct((orbitals, orbitals), jnp.float32)
    density = call(
        functools.partial(green_kernel, 1.0 / (members * blocks)),
        square,
        (left, steps, walkers),
        [
            pltpu.VMEM((members, electrons, orbitals), jnp.float32),
            pltpu.VMEM((members, electrons, electrons), jnp.float32),
            pltpu.VMEM((members, electrons, electrons), jnp.float32),
        ],
    )
    return lax.all_gather(total_over(density, "block"), "member")


def solution(mesh):
    sections, walks = mesh.devices.shape

    def run(fields, cholesky_vectors, trial_state, deviation):
        members = deviation.shape[1] // walks
        split_mesh = Mesh(
            mesh.devices.reshape(sections // members, members, walks),
            ("block", "member", "walk"),
        )
        section = ("block", "member")
        in_specs = (
            P(section, None, "walk"),
            P("walk", None, None),
            P(),
            P(section, "walk", None, None),
        )
        return jax.shard_map(
            body, mesh=split_mesh, in_specs=in_specs, out_specs=P("walk", None, None),
            check_vma=False,
        )(fields, cholesky_vectors, trial_state, deviation)

    return run
```

```python
import functools

import jax
import jax.numpy as jnp
from jax import lax
from jax.experimental import pallas as pl
from jax.experimental.pallas import tpu as pltpu
from jax.sharding import Mesh, PartitionSpec as P


SUB = 8
LANES = 128
DEPTH = 4
LAG = 4
CHUNKS = 5
ROUGH_STEPS = 24
ROUGH_REST = 0.05
MESH = pl.DeviceIdType.MESH


def split(a):
    high = a.astype(jnp.bfloat16)
    return high, (a - high.astype(jnp.float32)).astype(jnp.bfloat16)


def dot_f32(a, b):
    return jnp.dot(a, b, preferred_element_type=jnp.float32)


def dot3(a, b):
    a_high, a_low = split(a)
    b_high, b_low = split(b)
    return dot_f32(a_high, b_high) + (dot_f32(a_high, b_low) + dot_f32(a_low, b_high))


def greet(peers):
    barrier = pltpu.get_barrier_semaphore()
    for axis, peer in peers:
        pl.semaphore_signal(barrier, inc=1, device_id={axis: peer}, device_id_type=MESH)
    return barrier


def fold_rows(orbitals):
    return (orbitals // SUB + 1) // 2 * SUB


def contract_kernel(
    field_hbm, table_ref, trial_hbm, deviation_hbm, packed_ref, walkers_ref, flipped_ref,
    field_ref, trial_ref, deviation_ref, factor, low, high, part, arrived, total, gathered, walk_send, walk_recv,
    in_sem, low_sem, high_sem, x_send, x_recv, m_send, m_recv, w_send, w_recv,
):
    rows, chol = field_ref.shape
    per, orbitals, electrons = deviation_ref.shape
    members, walks = lax.axis_size("member"), lax.axis_size("walk")
    member, walk = lax.axis_index("member"), lax.axis_index("walk")
    half = fold_rows(orbitals)
    bands, folds = orbitals // SUB, half // SUB
    depth = chol * SUB
    order = [band for f in range(folds) for band in (f, f + folds) if band < bands]

    def fetch(place):
        band, slot = order[place], place % DEPTH
        at = pl.ds(band * SUB, SUB)
        copies = [
            pltpu.make_async_copy(
                table_ref.at[:, at, pl.ds(LANES, orbitals - LANES)], high.at[slot], high_sem.at[slot]
            )
        ]
        if band * SUB < LANES:
            copies.append(
                pltpu.make_async_copy(
                    table_ref.at[:, at, pl.ds(0, LANES)], low.at[slot], low_sem.at[slot]
                )
            )
        return copies

    flight = {}

    def start(place):
        if place < len(order):
            flight[place] = fetch(place)
            for copy in flight[place]:
                copy.start()

    inputs = [
        pltpu.make_async_copy(source, target, in_sem.at[i])
        for i, (source, target) in enumerate(
            [(field_hbm, field_ref), (trial_hbm, trial_ref), (deviation_hbm, deviation_ref)]
        )
    ]
    for copy in inputs:
        copy.start()
    for place in range(DEPTH):
        start(place)
    barrier = greet(
        [("walk", lax.rem(walk + s, walks)) for s in range(1, walks)]
        + [("member", lax.rem(member + s, members)) for s in range(1, members)]
    )
    inputs[0].wait()

    vector = lax.broadcasted_iota(jnp.int32, (chol, LANES), 0)
    lane = lax.broadcasted_iota(jnp.int32, (chol, LANES), 1)
    keep = lax.broadcasted_iota(jnp.int32, (2 * SUB, LANES), 0) % SUB
    keep = keep == lax.broadcasted_iota(jnp.int32, (2 * SUB, LANES), 1) % SUB
    for j in range(pl.cdiv(depth, LANES)):
        width = min(LANES, depth - j * LANES)
        pick = jnp.where(vector == j * (LANES // SUB) + lane // SUB, 1.0, 0.0)
        spread = dot_f32(field_ref[...], pick.astype(jnp.bfloat16))
        for row in range(0, rows, 2):
            pair = jnp.concatenate(
                [
                    jnp.broadcast_to(spread[row + i : row + i + 1], (SUB, LANES))
                    for i in range(2)
                ],
                axis=0,
            )
            factor[row * SUB : (row + 2) * SUB, j * LANES : j * LANES + width] = jnp.where(
                keep, pair, 0.0
            ).astype(jnp.bfloat16)[:, :width]

    for copy in inputs[1:]:
        copy.wait()
    walk_send[...] = trial_ref[...] + deviation_ref[...].astype(jnp.float32)
    flipped_ref[...] = jnp.zeros_like(flipped_ref)
    flipped_ref[:electrons, :] = trial_ref[...].T

    def product(place):
        band, slot = order[place], place % DEPTH
        for copy in flight[place]:
            copy.wait()
        right = dot_f32(factor[...], high[slot].reshape(depth, orbitals - LANES))
        right = right.reshape(rows, SUB, orbitals - LANES)
        left = None
        if band * SUB < LANES:
            left = dot_f32(factor[...], low[slot].reshape(depth, LANES))
            left = left.reshape(rows, SUB, LANES)
        return left, right

    def x_copy(shift, f):
        peer = lax.rem(walk + shift, walks)
        at = pl.ds(f * SUB, SUB)
        return pltpu.make_async_remote_copy(
            src_ref=part.at[pl.ds(peer * per, per), at, :],
            dst_ref=arrived.at[shift - 1, :, at, :],
            send_sem=x_send.at[shift - 1, f],
            recv_sem=x_recv.at[shift - 1, f],
            device_id={"walk": peer},
            device_id_type=MESH,
        )

    def m_copy(shift, f):
        peer = lax.rem(member + shift, members)
        at = pl.ds(f * SUB, SUB)
        return pltpu.make_async_remote_copy(
            src_ref=total.at[peer, at, :],
            dst_ref=gathered.at[member, at, :],
            send_sem=m_send.at[shift - 1, f],
            recv_sem=m_recv.at[shift - 1, f],
            device_id={"member": peer},
            device_id_type=MESH,
        )

    def w_copy(shift):
        peer = lax.rem(member + shift, members)
        return pltpu.make_async_remote_copy(
            src_ref=walk_send.at[peer],
            dst_ref=walk_recv.at[member],
            send_sem=w_send.at[shift - 1],
            recv_sem=w_recv.at[shift - 1],
            device_id={"member": peer},
            device_id_type=MESH,
        )

    def merge(f):
        at = slice(f * SUB, (f + 1) * SUB)
        value = part[pl.ds(walk * per, per), at, :]
        for shift in range(1, walks):
            x_copy(shift, f).wait_recv()
            value = value + arrived[shift - 1, :, at, :]
        total[:, at, :] = value

    sub = lax.broadcasted_iota(jnp.int32, (SUB, orbitals), 0)
    column = lax.broadcasted_iota(jnp.int32, (SUB, orbitals), 1)
    place = 0
    for f in range(folds + LAG + 1):
        if f < folds:
            left, right = product(place)
            start(place + DEPTH)
            place += 1
            upper = jnp.concatenate([left, right], axis=2)
            if f + folds < bands:
                left, right = product(place)
                start(place + DEPTH)
                place += 1
                if left is not None:
                    right = jnp.concatenate([left[:, :, half:], right], axis=2)
                    pad = 0
                else:
                    pad = LANES - half
                pieces = [right, jnp.zeros((rows, SUB, half), jnp.float32)]
                if pad:
                    pieces = [jnp.zeros((rows, SUB, pad), jnp.float32)] + pieces
                lower = jnp.concatenate(pieces, axis=2)
            else:
                lower = jnp.zeros_like(upper)
            own = (column >= half) | (column < f * SUB + sub)
            part[:, f * SUB : (f + 1) * SUB, :] = jnp.where(own[None], upper, lower)
        if f == 0:
            pl.semaphore_wait(barrier, walks + members - 2)
            for shift in range(1, members):
                w_copy(shift).start()
        if 1 <= f <= folds:
            for shift in range(1, walks):
                x_copy(shift, f - 1).start()
        if f > LAG:
            for shift in range(1, members):
                m_copy(shift, f - LAG - 1).start()
        if f >= LAG and f - LAG < folds:
            merge(f - LAG)
    packed_ref[member] = total[member]
    walkers_ref[member] = walk_send[member]
    for shift in range(1, members):
        source = lax.rem(member + members - shift, members)
        w_copy(shift).wait()
        walkers_ref[source] = walk_recv[source]
        for f in range(folds):
            m_copy(shift, f).wait()
        packed_ref[source] = gathered[source]
    for shift in range(1, walks):
        for f in range(folds):
            x_copy(shift, f).wait_send()


def contract(field_rows, cholesky_vectors, trial_state, deviation):
    rows, chol = field_rows.shape
    per, orbitals, electrons = deviation.shape
    members, walks = lax.axis_size("member"), lax.axis_size("walk")
    half = fold_rows(orbitals)
    folds = half // SUB
    vmem = pl.BlockSpec(memory_space=pltpu.VMEM)
    f32, bf16, dma = jnp.float32, jnp.bfloat16, pltpu.SemaphoreType.DMA
    return pl.pallas_call(
        contract_kernel,
        in_specs=[pl.BlockSpec(memory_space=pl.ANY)] * 4,
        out_specs=[vmem] * 3,
        out_shape=[
            jax.ShapeDtypeStruct((members, half, orbitals), f32),
            jax.ShapeDtypeStruct((members, orbitals, electrons), f32),
            jax.ShapeDtypeStruct((-(-electrons // SUB) * SUB, orbitals), f32),
        ],
        scratch_shapes=[
            pltpu.VMEM((rows, chol), bf16),
            pltpu.VMEM((orbitals, electrons), f32),
            pltpu.VMEM((per, orbitals, electrons), bf16),
            pltpu.VMEM((rows * SUB, chol * SUB), bf16),
            pltpu.VMEM((DEPTH, chol, SUB, LANES), bf16),
            pltpu.VMEM((DEPTH, chol, SUB, orbitals - LANES), bf16),
            pltpu.VMEM((rows, half, orbitals), f32),
            pltpu.VMEM((walks - 1, per, half, orbitals), f32),
            pltpu.VMEM((per, half, orbitals), f32),
            pltpu.VMEM((members, half, orbitals), f32),
            pltpu.VMEM((per, orbitals, electrons), f32),
            pltpu.VMEM((members, orbitals, electrons), f32),
            dma((3,)),
            dma((DEPTH,)),
            dma((DEPTH,)),
            dma((walks - 1, folds)),
            dma((walks - 1, folds)),
            dma((members - 1, folds)),
            dma((members - 1, folds)),
            dma((members - 1,)),
            dma((members - 1,)),
        ],
        compiler_params=pltpu.CompilerParams(
            vmem_limit_bytes=48 * 2**20, collective_id=0, has_side_effects=True
        ),
    )(field_rows, cholesky_vectors, trial_state, deviation)


def eye(size):
    row = lax.broadcasted_iota(jnp.int32, (size, size), 0)
    column = lax.broadcasted_iota(jnp.int32, (size, size), 1)
    return jnp.where(row == column, 1.0, 0.0)


def unfold(packed):
    half, orbitals = packed.shape
    rest = orbitals - half
    row = lax.broadcasted_iota(jnp.int32, (half, half), 0)
    column = lax.broadcasted_iota(jnp.int32, (half, half), 1)
    square = packed[:, :half]
    flipped = -square.T
    first = jnp.where(row > column, square, jnp.where(row < column, flipped, 0.0))
    second = jnp.where(row < column, square, jnp.where(row > column, flipped, 0.0))
    across = packed[:, half:]
    return jnp.concatenate(
        [
            jnp.concatenate([first, across], axis=1),
            jnp.concatenate([-across.T, second[:rest, :rest]], axis=1),
        ],
        axis=0,
    )


def series(v, unit):
    v2 = dot3(v, v)
    v3 = dot3(v2, v)
    upper = unit * (1 / 6) + v * (1 / 24) + v2 * (1 / 120) + v3 * (1 / 720)
    return (unit + v + v2 * 0.5) + dot3(v3, upper)


def chain_kernel(packed_ref, trial_ref, steps_ref, left_ref, held, sent, send_sem, recv_sem):
    members = packed_ref.shape[0]
    padded, orbitals = held.shape
    blocks, block = lax.axis_size("block"), lax.axis_index("block")
    has_next, has_last = block < blocks - 1, block > 0
    cuts = [0, (padded // SUB + 1) // 2 * SUB, padded]
    barrier = pltpu.get_barrier_semaphore()
    for near, step in ((has_next, 1), (has_last, -1)):
        @pl.when(near)
        def _():
            pl.semaphore_signal(
                barrier, inc=1, device_id={"block": block + step}, device_id_type=MESH
            )

    unit = eye(orbitals)
    for s in range(members):
        steps_ref[s] = series(unfold(packed_ref[s]), unit)
    parts = [steps_ref[s] for s in reversed(range(members))]
    while len(parts) > 1:
        paired = [dot3(parts[i], parts[i + 1]) for i in range(0, len(parts) - 1, 2)]
        parts = paired + parts[len(parts) - len(parts) % 2 :]
    step_map = parts[0]
    pl.semaphore_wait(barrier, has_next.astype(jnp.int32) + has_last.astype(jnp.int32))

    def copy(i):
        at = pl.ds(cuts[i], cuts[i + 1] - cuts[i])
        return pltpu.make_async_remote_copy(
            src_ref=sent.at[at, :],
            dst_ref=held.at[at, :],
            send_sem=send_sem.at[i],
            recv_sem=recv_sem.at[i],
            device_id={"block": lax.rem(block + blocks - 1, blocks)},
            device_id_type=MESH,
        )

    @pl.when(jnp.logical_not(has_next))
    def _():
        held[...] = trial_ref[...]

    for i in range(len(cuts) - 1):
        @pl.when(has_next)
        def _():
            copy(i).wait_recv()

        @pl.when(has_last)
        def _():
            at = slice(cuts[i], cuts[i + 1])
            sent[at, :] = dot3(held[at, :], step_map)
            copy(i).start()

    left_ref[...] = held[: left_ref.shape[0], :]

    @pl.when(has_last)
    def _():
        for i in range(len(cuts) - 1):
            copy(i).wait_send()


def chain(packed, trial, electrons):
    members = packed.shape[0]
    padded, orbitals = trial.shape
    vmem = pl.BlockSpec(memory_space=pltpu.VMEM)
    return pl.pallas_call(
        chain_kernel,
        in_specs=[vmem, vmem],
        out_specs=[vmem, vmem],
        out_shape=[
            jax.ShapeDtypeStruct((members, orbitals, orbitals), jnp.float32),
            jax.ShapeDtypeStruct((electrons, orbitals), jnp.float32),
        ],
        scratch_shapes=[
            pltpu.VMEM((padded, orbitals), jnp.float32),
            pltpu.VMEM((padded, orbitals), jnp.float32),
            pltpu.SemaphoreType.DMA((2,)),
            pltpu.SemaphoreType.DMA((2,)),
        ],
        compiler_params=pltpu.CompilerParams(
            vmem_limit_bytes=48 * 2**20, collective_id=1, has_side_effects=True
        ),
    )(packed, trial)


def green_kernel(
    scale, left_in_ref, steps_ref, walk_ref, out_ref, left_ref, inter_ref, inverse_ref, first_ref
):
    members = steps_ref.shape[0]
    unit = eye(left_in_ref.shape[0])
    left = left_in_ref[...]
    for s in reversed(range(members)):
        left = dot3(left, steps_ref[s])
        left_ref[s] = left
    for s in range(members):
        inter = dot3(left_ref[s], walk_ref[s])
        inter_ref[s] = inter
        flipped = inter.T
        square = dot3(inter, flipped)
        inverse_ref[s] = flipped * lax.rsqrt(jnp.sum(square * square))

    def newton(dot):
        worst = jnp.float32(0.0)
        for s in range(members):
            guess = inverse_ref[s]
            rest = unit - dot(inter_ref[s], guess)
            inverse_ref[s] = guess + dot(guess, rest)
            worst = jnp.maximum(worst, jnp.sum(rest * rest))
        return worst

    def rounded(a, b):
        return dot_f32(a.astype(jnp.bfloat16), b.astype(jnp.bfloat16))

    for s in range(members):
        first_ref[s] = inverse_ref[s]
    size = unit.shape[0]
    _, rough = lax.while_loop(
        lambda state: (state[0] < ROUGH_STEPS) & (state[1] > ROUGH_REST),
        lambda state: (state[0] + 1, newton(rounded)),
        (jnp.int32(0), jnp.float32(size)),
    )

    @pl.when(jnp.logical_not(rough <= ROUGH_REST))
    def _():
        for s in range(members):
            inverse_ref[s] = first_ref[s]

    lax.while_loop(
        lambda state: (state[0] < 80) & (state[1] > 1e-4),
        lambda state: (state[0] + 1, newton(dot3)),
        (jnp.int32(0), jnp.float32(1.0)),
    )
    newton(dot3)
    total = None
    for s in range(members):
        green = dot3(walk_ref[s], dot3(inverse_ref[s], left_ref[s]))
        total = green if total is None else total + green
    out_ref[...] = total * scale


def call(kernel, out_shape, args, scratch=(), scalars=0):
    vmem = pl.BlockSpec(memory_space=pltpu.VMEM)
    smem = pl.BlockSpec(memory_space=pltpu.SMEM)
    return pl.pallas_call(
        kernel,
        in_specs=[smem] * scalars + [vmem] * (len(args) - scalars),
        out_specs=vmem,
        out_shape=out_shape,
        scratch_shapes=list(scratch),
        compiler_params=pltpu.CompilerParams(vmem_limit_bytes=48 * 2**20),
    )(*args)


def spread_kernel(density_ref, out_ref, falling, arrived, whole, *sems):
    up_send, up_recv, down_send, down_recv, near_send, near_recv = sems
    orbitals = density_ref.shape[0]
    blocks, members = lax.axis_size("block"), lax.axis_size("member")
    block, member = lax.axis_index("block"), lax.axis_index("member")
    has_next, has_last = block < blocks - 1, block > 0
    bits = [1 << i for i in reversed(range(members.bit_length() - 1))]
    offsets, pairs = [0], []
    for bit in bits:
        pairs += [(bit, offset) for offset in offsets]
        offsets += [offset + bit for offset in offsets]
    came = {bit + offset: j for j, (bit, offset) in enumerate(pairs)}
    bands = pl.cdiv(orbitals, SUB)
    cuts = [c * bands // CHUNKS * SUB for c in range(CHUNKS)] + [orbitals]
    after, before = lax.rem(block + 1, blocks), lax.rem(block + blocks - 1, blocks)

    def flip(offset):
        place = member
        for bit in bits:
            if offset & bit:
                place = place + bit - 2 * bit * ((place // bit) % 2)
        return place

    def remote(source, target, send, recv, device):
        return pltpu.make_async_remote_copy(
            src_ref=source, dst_ref=target, send_sem=send, recv_sem=recv,
            device_id=device, device_id_type=MESH,
        )

    def rows(c):
        return pl.ds(cuts[c], cuts[c + 1] - cuts[c])

    def fall(c):
        return remote(
            falling.at[rows(c), :], arrived.at[rows(c), :],
            down_send.at[c], down_recv.at[c], {"block": before},
        )

    def rise(c):
        piece = whole.at[member, rows(c), :]
        return remote(piece, piece, up_send.at[c], up_recv.at[c], {"block": after})

    def near(j, c):
        bit, offset = pairs[j]
        piece = whole.at[flip(offset), rows(c), :]
        return remote(
            piece, piece, near_send.at[j, c], near_recv.at[j, c], {"member": flip(bit)}
        )

    barrier = pltpu.get_barrier_semaphore()
    for has, peer in ((has_next, after), (has_last, before)):
        @pl.when(has)
        def _():
            pl.semaphore_signal(barrier, inc=1, device_id={"block": peer}, device_id_type=MESH)

    for bit in bits:
        pl.semaphore_signal(
            barrier, inc=1, device_id={"member": flip(bit)}, device_id_type=MESH
        )
    pl.semaphore_wait(
        barrier, has_next.astype(jnp.int32) + has_last.astype(jnp.int32) + len(bits)
    )
    for c in range(CHUNKS):
        at = slice(cuts[c], cuts[c + 1])
        falling[at, :] = density_ref[at, :]

        @pl.when(has_next)
        def _():
            fall(c).wait_recv()
            falling[at, :] += arrived[at, :]

        @pl.when(has_last)
        def _():
            fall(c).start()

        @pl.when(jnp.logical_not(has_last))
        def _():
            whole[member, at, :] = falling[at, :]

    waited = set()
    for step in range(CHUNKS + len(bits)):
        if step < CHUNKS:
            @pl.when(has_last)
            def _():
                rise(step).wait_recv()

            @pl.when(has_next)
            def _():
                rise(step).start()

        for j, (bit, offset) in enumerate(pairs):
            c = step - offset.bit_count()
            if not 0 <= c < CHUNKS:
                continue
            if offset and (came[offset], c) not in waited:
                near(came[offset], c).wait_recv()
                waited.add((came[offset], c))
            near(j, c).start()
    for j in range(len(pairs)):
        for c in range(CHUNKS):
            if (j, c) not in waited:
                near(j, c).wait_recv()
    out_ref[...] = whole[...]
    for c in range(CHUNKS):
        for j in range(len(pairs)):
            near(j, c).wait_send()

        @pl.when(has_last)
        def _():
            fall(c).wait_send()

        @pl.when(has_next)
        def _():
            rise(c).wait_send()


def spread(density):
    members = lax.axis_size("member")
    if members & (members - 1):
        return lax.all_gather(lax.psum(density, "block"), "member")
    orbitals = density.shape[0]
    vmem, dma = pl.BlockSpec(memory_space=pltpu.VMEM), pltpu.SemaphoreType.DMA
    every = (members, orbitals, orbitals)
    return pl.pallas_call(
        spread_kernel,
        in_specs=[vmem],
        out_specs=vmem,
        out_shape=jax.ShapeDtypeStruct(every, jnp.float32),
        scratch_shapes=[
            pltpu.VMEM((orbitals, orbitals), jnp.float32),
            pltpu.VMEM((orbitals, orbitals), jnp.float32),
            pltpu.VMEM(every, jnp.float32),
        ]
        + [dma((CHUNKS,))] * 4
        + [dma((members - 1, CHUNKS))] * 2,
        compiler_params=pltpu.CompilerParams(
            vmem_limit_bytes=48 * 2**20, collective_id=2, has_side_effects=True
        ),
    )(density)


def body(fields, cholesky_vectors, trial_state, deviation):
    chol = fields.shape[2]
    orbitals, electrons = trial_state.shape
    blocks, members = lax.axis_size("block"), lax.axis_size("member")
    packed, walkers, trial = contract(
        fields.reshape(-1, chol), cholesky_vectors, trial_state, deviation[0]
    )
    steps, left = chain(packed, trial, electrons)
    square = jax.ShapeDtypeStruct((orbitals, orbitals), jnp.float32)
    density = call(
        functools.partial(green_kernel, 1.0 / (members * blocks)),
        square,
        (left, steps, walkers),
        [pltpu.VMEM((members, electrons, orbitals), jnp.float32)]
        + [pltpu.VMEM((members, electrons, electrons), jnp.float32)] * 3,
    )
    return spread(density)


def solution(mesh):
    sections, walks = mesh.devices.shape

    def run(fields, cholesky_vectors, trial_state, deviation):
        members = deviation.shape[1] // walks
        split_mesh = Mesh(
            mesh.devices.reshape(sections // members, members, walks),
            ("block", "member", "walk"),
        )
        section = ("block", "member")
        in_specs = (
            P(section, None, "walk"),
            P("walk", None, None),
            P(),
            P(section, "walk", None, None),
        )
        return jax.shard_map(
            body, mesh=split_mesh, in_specs=in_specs, out_specs=P("walk", None, None),
            check_vma=False,
        )(fields, cholesky_vectors, trial_state, deviation)

    return run
```

```python
import functools

import jax
import jax.numpy as jnp
from jax import lax
from jax.experimental import pallas as pl
from jax.experimental.pallas import tpu as pltpu
from jax.sharding import Mesh, PartitionSpec as P


SUB = 8
LANES = 128
DEPTH = 4
LAG = 4
ROUGH_STEPS = 24
ROUGH_REST = 0.05
MESH = pl.DeviceIdType.MESH


def split(a):
    high = a.astype(jnp.bfloat16)
    return high, (a - high.astype(jnp.float32)).astype(jnp.bfloat16)


def dot_f32(a, b):
    return jnp.dot(a, b, preferred_element_type=jnp.float32)


def dot3(a, b):
    a_high, a_low = split(a)
    b_high, b_low = split(b)
    return dot_f32(a_high, b_high) + (dot_f32(a_high, b_low) + dot_f32(a_low, b_high))


def greet(peers):
    barrier = pltpu.get_barrier_semaphore()
    for axis, peer in peers:
        pl.semaphore_signal(barrier, inc=1, device_id={axis: peer}, device_id_type=MESH)
    return barrier


def fold_rows(orbitals):
    return (orbitals // SUB + 1) // 2 * SUB


def contract_kernel(
    field_hbm, table_ref, trial_hbm, deviation_hbm, packed_ref, walkers_ref, flipped_ref,
    field_ref, trial_ref, deviation_ref, factor, low, high, part, arrived, total, gathered, walk_send, walk_recv,
    in_sem, low_sem, high_sem, x_send, x_recv, m_send, m_recv, w_send, w_recv,
):
    rows, chol = field_ref.shape
    per, orbitals, electrons = deviation_ref.shape
    members, walks = lax.axis_size("member"), lax.axis_size("walk")
    member, walk = lax.axis_index("member"), lax.axis_index("walk")
    half = fold_rows(orbitals)
    bands, folds = orbitals // SUB, half // SUB
    depth = chol * SUB
    order = [band for f in range(folds) for band in (f, f + folds) if band < bands]

    def fetch(place):
        band, slot = order[place], place % DEPTH
        at = pl.ds(band * SUB, SUB)
        copies = [
            pltpu.make_async_copy(
                table_ref.at[:, at, pl.ds(LANES, orbitals - LANES)], high.at[slot], high_sem.at[slot]
            )
        ]
        if band * SUB < LANES:
            copies.append(
                pltpu.make_async_copy(
                    table_ref.at[:, at, pl.ds(0, LANES)], low.at[slot], low_sem.at[slot]
                )
            )
        return copies

    flight = {}

    def start(place):
        if place < len(order):
            flight[place] = fetch(place)
            for copy in flight[place]:
                copy.start()

    inputs = [
        pltpu.make_async_copy(source, target, in_sem.at[i])
        for i, (source, target) in enumerate(
            [(field_hbm, field_ref), (trial_hbm, trial_ref), (deviation_hbm, deviation_ref)]
        )
    ]
    for copy in inputs:
        copy.start()
    for place in range(DEPTH):
        start(place)
    barrier = greet(
        [("walk", lax.rem(walk + s, walks)) for s in range(1, walks)]
        + [("member", lax.rem(member + s, members)) for s in range(1, members)]
    )
    inputs[0].wait()

    vector = lax.broadcasted_iota(jnp.int32, (chol, LANES), 0)
    lane = lax.broadcasted_iota(jnp.int32, (chol, LANES), 1)
    keep = lax.broadcasted_iota(jnp.int32, (2 * SUB, LANES), 0) % SUB
    keep = keep == lax.broadcasted_iota(jnp.int32, (2 * SUB, LANES), 1) % SUB
    for j in range(pl.cdiv(depth, LANES)):
        width = min(LANES, depth - j * LANES)
        pick = jnp.where(vector == j * (LANES // SUB) + lane // SUB, 1.0, 0.0)
        spread = dot_f32(field_ref[...], pick.astype(jnp.bfloat16))
        for row in range(0, rows, 2):
            pair = jnp.concatenate(
                [
                    jnp.broadcast_to(spread[row + i : row + i + 1], (SUB, LANES))
                    for i in range(2)
                ],
                axis=0,
            )
            factor[row * SUB : (row + 2) * SUB, j * LANES : j * LANES + width] = jnp.where(
                keep, pair, 0.0
            ).astype(jnp.bfloat16)[:, :width]

    for copy in inputs[1:]:
        copy.wait()
    walk_send[...] = trial_ref[...] + deviation_ref[...].astype(jnp.float32)
    flipped_ref[...] = jnp.zeros_like(flipped_ref)
    flipped_ref[:electrons, :] = trial_ref[...].T

    def product(place):
        band, slot = order[place], place % DEPTH
        for copy in flight[place]:
            copy.wait()
        right = dot_f32(factor[...], high[slot].reshape(depth, orbitals - LANES))
        right = right.reshape(rows, SUB, orbitals - LANES)
        left = None
        if band * SUB < LANES:
            left = dot_f32(factor[...], low[slot].reshape(depth, LANES))
            left = left.reshape(rows, SUB, LANES)
        return left, right

    def x_copy(shift, f):
        peer = lax.rem(walk + shift, walks)
        at = pl.ds(f * SUB, SUB)
        return pltpu.make_async_remote_copy(
            src_ref=part.at[pl.ds(peer * per, per), at, :],
            dst_ref=arrived.at[shift - 1, :, at, :],
            send_sem=x_send.at[shift - 1, f],
            recv_sem=x_recv.at[shift - 1, f],
            device_id={"walk": peer},
            device_id_type=MESH,
        )

    def m_copy(shift, f):
        peer = lax.rem(member + shift, members)
        at = pl.ds(f * SUB, SUB)
        return pltpu.make_async_remote_copy(
            src_ref=total.at[peer, at, :],
            dst_ref=gathered.at[member, at, :],
            send_sem=m_send.at[shift - 1, f],
            recv_sem=m_recv.at[shift - 1, f],
            device_id={"member": peer},
            device_id_type=MESH,
        )

    def w_copy(shift):
        peer = lax.rem(member + shift, members)
        return pltpu.make_async_remote_copy(
            src_ref=walk_send.at[peer],
            dst_ref=walk_recv.at[member],
            send_sem=w_send.at[shift - 1],
            recv_sem=w_recv.at[shift - 1],
            device_id={"member": peer},
            device_id_type=MESH,
        )

    def merge(f):
        at = slice(f * SUB, (f + 1) * SUB)
        value = part[pl.ds(walk * per, per), at, :]
        for shift in range(1, walks):
            x_copy(shift, f).wait_recv()
            value = value + arrived[shift - 1, :, at, :]
        total[:, at, :] = value

    sub = lax.broadcasted_iota(jnp.int32, (SUB, orbitals), 0)
    column = lax.broadcasted_iota(jnp.int32, (SUB, orbitals), 1)
    place = 0
    for f in range(folds + LAG + 1):
        if f < folds:
            left, right = product(place)
            start(place + DEPTH)
            place += 1
            upper = jnp.concatenate([left, right], axis=2)
            if f + folds < bands:
                left, right = product(place)
                start(place + DEPTH)
                place += 1
                if left is not None:
                    right = jnp.concatenate([left[:, :, half:], right], axis=2)
                    pad = 0
                else:
                    pad = LANES - half
                pieces = [right, jnp.zeros((rows, SUB, half), jnp.float32)]
                if pad:
                    pieces = [jnp.zeros((rows, SUB, pad), jnp.float32)] + pieces
                lower = jnp.concatenate(pieces, axis=2)
            else:
                lower = jnp.zeros_like(upper)
            own = (column >= half) | (column < f * SUB + sub)
            part[:, f * SUB : (f + 1) * SUB, :] = jnp.where(own[None], upper, lower)
        if f == 0:
            pl.semaphore_wait(barrier, walks + members - 2)
            for shift in range(1, members):
                w_copy(shift).start()
        if 1 <= f <= folds:
            for shift in range(1, walks):
                x_copy(shift, f - 1).start()
        if f > LAG:
            for shift in range(1, members):
                m_copy(shift, f - LAG - 1).start()
        if f >= LAG and f - LAG < folds:
            merge(f - LAG)
    packed_ref[member] = total[member]
    walkers_ref[member] = walk_send[member]
    for shift in range(1, members):
        source = lax.rem(member + members - shift, members)
        w_copy(shift).wait()
        walkers_ref[source] = walk_recv[source]
        for f in range(folds):
            m_copy(shift, f).wait()
        packed_ref[source] = gathered[source]
    for shift in range(1, walks):
        for f in range(folds):
            x_copy(shift, f).wait_send()


def contract(field_rows, cholesky_vectors, trial_state, deviation):
    rows, chol = field_rows.shape
    per, orbitals, electrons = deviation.shape
    members, walks = lax.axis_size("member"), lax.axis_size("walk")
    half = fold_rows(orbitals)
    folds = half // SUB
    vmem = pl.BlockSpec(memory_space=pltpu.VMEM)
    f32, bf16, dma = jnp.float32, jnp.bfloat16, pltpu.SemaphoreType.DMA
    return pl.pallas_call(
        contract_kernel,
        in_specs=[pl.BlockSpec(memory_space=pltpu.HBM)] * 4,
        out_specs=[vmem] * 3,
        out_shape=[
            jax.ShapeDtypeStruct((members, half, orbitals), f32),
            jax.ShapeDtypeStruct((members, orbitals, electrons), f32),
            jax.ShapeDtypeStruct((-(-electrons // SUB) * SUB, orbitals), f32),
        ],
        scratch_shapes=[
            pltpu.VMEM((rows, chol), bf16),
            pltpu.VMEM((orbitals, electrons), f32),
            pltpu.VMEM((per, orbitals, electrons), bf16),
            pltpu.VMEM((rows * SUB, chol * SUB), bf16),
            pltpu.VMEM((DEPTH, chol, SUB, LANES), bf16),
            pltpu.VMEM((DEPTH, chol, SUB, orbitals - LANES), bf16),
            pltpu.VMEM((rows, half, orbitals), f32),
            pltpu.VMEM((walks - 1, per, half, orbitals), f32),
            pltpu.VMEM((per, half, orbitals), f32),
            pltpu.VMEM((members, half, orbitals), f32),
            pltpu.VMEM((per, orbitals, electrons), f32),
            pltpu.VMEM((members, orbitals, electrons), f32),
            dma((3,)),
            dma((DEPTH,)),
            dma((DEPTH,)),
            dma((walks - 1, folds)),
            dma((walks - 1, folds)),
            dma((members - 1, folds)),
            dma((members - 1, folds)),
            dma((members - 1,)),
            dma((members - 1,)),
        ],
        compiler_params=pltpu.CompilerParams(
            vmem_limit_bytes=48 * 2**20, collective_id=0, has_side_effects=True
        ),
    )(field_rows, cholesky_vectors, trial_state, deviation)


def eye(size):
    row = lax.broadcasted_iota(jnp.int32, (size, size), 0)
    column = lax.broadcasted_iota(jnp.int32, (size, size), 1)
    return jnp.where(row == column, 1.0, 0.0)


def unfold(packed):
    half, orbitals = packed.shape
    rest = orbitals - half
    row = lax.broadcasted_iota(jnp.int32, (half, half), 0)
    column = lax.broadcasted_iota(jnp.int32, (half, half), 1)
    square = packed[:, :half]
    flipped = -square.T
    first = jnp.where(row > column, square, jnp.where(row < column, flipped, 0.0))
    second = jnp.where(row < column, square, jnp.where(row > column, flipped, 0.0))
    across = packed[:, half:]
    return jnp.concatenate(
        [
            jnp.concatenate([first, across], axis=1),
            jnp.concatenate([-across.T, second[:rest, :rest]], axis=1),
        ],
        axis=0,
    )


def series(v, unit):
    v2 = dot3(v, v)
    v3 = dot3(v2, v)
    upper = unit * (1 / 6) + v * (1 / 24) + v2 * (1 / 120) + v3 * (1 / 720)
    return (unit + v + v2 * 0.5) + dot3(v3, upper)


def chain_kernel(packed_ref, trial_ref, steps_ref, left_ref, held, sent, send_sem, recv_sem):
    members = packed_ref.shape[0]
    padded, orbitals = held.shape
    blocks, block = lax.axis_size("block"), lax.axis_index("block")
    has_next, has_last = block < blocks - 1, block > 0
    cuts = [0, (padded // SUB + 1) // 2 * SUB, padded]
    barrier = pltpu.get_barrier_semaphore()
    for near, step in ((has_next, 1), (has_last, -1)):
        @pl.when(near)
        def _():
            pl.semaphore_signal(
                barrier, inc=1, device_id={"block": block + step}, device_id_type=MESH
            )

    unit = eye(orbitals)
    for s in range(members):
        steps_ref[s] = series(unfold(packed_ref[s]), unit)
    parts = [steps_ref[s] for s in reversed(range(members))]
    while len(parts) > 1:
        paired = [dot3(parts[i], parts[i + 1]) for i in range(0, len(parts) - 1, 2)]
        parts = paired + parts[len(parts) - len(parts) % 2 :]
    step_map = parts[0]
    pl.semaphore_wait(barrier, has_next.astype(jnp.int32) + has_last.astype(jnp.int32))

    def copy(i):
        at = pl.ds(cuts[i], cuts[i + 1] - cuts[i])
        return pltpu.make_async_remote_copy(
            src_ref=sent.at[at, :],
            dst_ref=held.at[at, :],
            send_sem=send_sem.at[i],
            recv_sem=recv_sem.at[i],
            device_id={"block": lax.rem(block + blocks - 1, blocks)},
            device_id_type=MESH,
        )

    @pl.when(jnp.logical_not(has_next))
    def _():
        held[...] = trial_ref[...]

    for i in range(len(cuts) - 1):
        @pl.when(has_next)
        def _():
            copy(i).wait_recv()

        @pl.when(has_last)
        def _():
            at = slice(cuts[i], cuts[i + 1])
            sent[at, :] = dot3(held[at, :], step_map)
            copy(i).start()

    left_ref[...] = held[: left_ref.shape[0], :]

    @pl.when(has_last)
    def _():
        for i in range(len(cuts) - 1):
            copy(i).wait_send()


def chain(packed, trial, electrons):
    members = packed.shape[0]
    padded, orbitals = trial.shape
    vmem = pl.BlockSpec(memory_space=pltpu.VMEM)
    return pl.pallas_call(
        chain_kernel,
        in_specs=[vmem, vmem],
        out_specs=[vmem, vmem],
        out_shape=[
            jax.ShapeDtypeStruct((members, orbitals, orbitals), jnp.float32),
            jax.ShapeDtypeStruct((electrons, orbitals), jnp.float32),
        ],
        scratch_shapes=[
            pltpu.VMEM((padded, orbitals), jnp.float32),
            pltpu.VMEM((padded, orbitals), jnp.float32),
            pltpu.SemaphoreType.DMA((2,)),
            pltpu.SemaphoreType.DMA((2,)),
        ],
        compiler_params=pltpu.CompilerParams(
            vmem_limit_bytes=48 * 2**20, collective_id=1, has_side_effects=True
        ),
    )(packed, trial)


def green_kernel(
    scale, left_in_ref, steps_ref, walk_ref, out_ref, left_ref, inter_ref, inverse_ref, first_ref
):
    members = steps_ref.shape[0]
    unit = eye(left_in_ref.shape[0])
    left = left_in_ref[...]
    for s in reversed(range(members)):
        left = dot3(left, steps_ref[s])
        left_ref[s] = left
    for s in range(members):
        inter = dot3(left_ref[s], walk_ref[s])
        inter_ref[s] = inter
        flipped = inter.T
        square = dot3(inter, flipped)
        inverse_ref[s] = flipped * lax.rsqrt(jnp.sum(square * square))

    def newton(dot):
        worst = jnp.float32(0.0)
        for s in range(members):
            guess = inverse_ref[s]
            rest = unit - dot(inter_ref[s], guess)
            inverse_ref[s] = guess + dot(guess, rest)
            worst = jnp.maximum(worst, jnp.sum(rest * rest))
        return worst

    def rounded(a, b):
        return dot_f32(a.astype(jnp.bfloat16), b.astype(jnp.bfloat16))

    for s in range(members):
        first_ref[s] = inverse_ref[s]
    size = unit.shape[0]
    _, rough = lax.while_loop(
        lambda state: (state[0] < ROUGH_STEPS) & (state[1] > ROUGH_REST),
        lambda state: (state[0] + 1, newton(rounded)),
        (jnp.int32(0), jnp.float32(size)),
    )

    @pl.when(jnp.logical_not(rough <= ROUGH_REST))
    def _():
        for s in range(members):
            inverse_ref[s] = first_ref[s]

    lax.while_loop(
        lambda state: (state[0] < 80) & (state[1] > 1e-4),
        lambda state: (state[0] + 1, newton(dot3)),
        (jnp.int32(0), jnp.float32(1.0)),
    )
    newton(dot3)
    total = None
    for s in range(members):
        green = dot3(walk_ref[s], dot3(inverse_ref[s], left_ref[s]))
        total = green if total is None else total + green
    out_ref[...] = total * scale


def call(kernel, out_shape, args, scratch=(), scalars=0):
    vmem = pl.BlockSpec(memory_space=pltpu.VMEM)
    smem = pl.BlockSpec(memory_space=pltpu.SMEM)
    return pl.pallas_call(
        kernel,
        in_specs=[smem] * scalars + [vmem] * (len(args) - scalars),
        out_specs=vmem,
        out_shape=out_shape,
        scratch_shapes=list(scratch),
        compiler_params=pltpu.CompilerParams(vmem_limit_bytes=48 * 2**20),
    )(*args)


def spread_kernel(density_ref, out_ref, mine, arrived, whole, *sems):
    sum_send, sum_recv, all_send, all_recv, near_send, near_recv = sems
    orbitals = density_ref.shape[0]
    blocks, piece, _ = mine.shape
    members = whole.shape[0]
    block, member = lax.axis_index("block"), lax.axis_index("member")
    bits = [1 << i for i in reversed(range(members.bit_length() - 1))]
    offsets, pairs = [0], []
    for bit in bits:
        pairs += [(bit, offset) for offset in offsets]
        offsets += [offset + bit for offset in offsets]
    came = {bit + offset: j for j, (bit, offset) in enumerate(pairs)}
    shifts = sorted(range(1, blocks), key=lambda shift: min(shift, blocks - shift))

    def flip(offset):
        place = member
        for bit in bits:
            if offset & bit:
                place = place + bit - 2 * bit * ((place // bit) % 2)
        return place

    def remote(source, target, send, recv, device):
        return pltpu.make_async_remote_copy(
            src_ref=source, dst_ref=target, send_sem=send, recv_sem=recv,
            device_id=device, device_id_type=MESH,
        )

    def to_sum(shift):
        peer = lax.rem(block + shift, blocks)
        return remote(
            mine.at[peer], arrived.at[shift - 1],
            sum_send.at[shift - 1], sum_recv.at[shift - 1], {"block": peer},
        )

    def to_all(shift):
        ref = whole.at[member, block]
        return remote(
            ref, ref, all_send.at[shift - 1], all_recv.at[shift - 1],
            {"block": lax.rem(block + shift, blocks)},
        )

    def near(j, shift):
        bit, offset = pairs[j]
        ref = whole.at[flip(offset), lax.rem(block + blocks - shift, blocks)]
        return remote(
            ref, ref, near_send.at[j, shift], near_recv.at[j, shift], {"member": flip(bit)}
        )

    barrier = greet(
        [("block", lax.rem(block + shift, blocks)) for shift in shifts]
        + [("member", flip(bit)) for bit in bits]
    )
    for q in range(blocks):
        rows = min(piece, orbitals - q * piece)
        if rows > 0:
            mine[q, :rows, :] = density_ref[q * piece : q * piece + rows, :]
        if rows < piece:
            mine[q, max(rows, 0) :, :] = jnp.zeros((piece - max(rows, 0), orbitals), jnp.float32)
    pl.semaphore_wait(barrier, len(shifts) + len(bits))
    for shift in shifts:
        to_sum(shift).start()
    value = mine[block]
    for shift in shifts:
        to_sum(shift).wait_recv()
        value = value + arrived[shift - 1]
    whole[member, block] = value
    for shift in shifts:
        to_all(shift).start()
    for shift in [0] + shifts:
        if shift:
            to_all(shift).wait_recv()
        for j, (bit, offset) in enumerate(pairs):
            if not offset:
                near(j, shift).start()
    waited = set()
    for offset in offsets[1:]:
        for shift in [0] + shifts:
            for j, (bit, held) in enumerate(pairs):
                if held == offset:
                    if (came[offset], shift) not in waited:
                        near(came[offset], shift).wait_recv()
                        waited.add((came[offset], shift))
                    near(j, shift).start()
    for shift in [0] + shifts:
        for j in range(len(pairs)):
            if (j, shift) not in waited:
                near(j, shift).wait_recv()
    for q in range(blocks):
        rows = min(piece, orbitals - q * piece)
        if rows > 0:
            out_ref[:, q * piece : q * piece + rows, :] = whole[:, q, :rows, :]
    for shift in [0] + shifts:
        if shift:
            to_sum(shift).wait_send()
            to_all(shift).wait_send()
        for j in range(len(pairs)):
            near(j, shift).wait_send()


def spread(density):
    blocks, members = lax.axis_size("block"), lax.axis_size("member")
    if members & (members - 1):
        return lax.all_gather(lax.psum(density, "block"), "member")
    orbitals = density.shape[0]
    piece = pl.cdiv(pl.cdiv(orbitals, SUB), blocks) * SUB
    vmem, dma = pl.BlockSpec(memory_space=pltpu.VMEM), pltpu.SemaphoreType.DMA
    return pl.pallas_call(
        spread_kernel,
        in_specs=[vmem],
        out_specs=vmem,
        out_shape=jax.ShapeDtypeStruct((members, orbitals, orbitals), jnp.float32),
        scratch_shapes=[
            pltpu.VMEM((blocks, piece, orbitals), jnp.float32),
            pltpu.VMEM((blocks - 1, piece, orbitals), jnp.float32),
            pltpu.VMEM((members, blocks, piece, orbitals), jnp.float32),
        ]
        + [dma((blocks - 1,))] * 4
        + [dma((members - 1, blocks))] * 2,
        compiler_params=pltpu.CompilerParams(
            vmem_limit_bytes=48 * 2**20, collective_id=2, has_side_effects=True
        ),
    )(density)


def body(fields, cholesky_vectors, trial_state, deviation):
    chol = fields.shape[2]
    orbitals, electrons = trial_state.shape
    blocks, members = lax.axis_size("block"), lax.axis_size("member")
    packed, walkers, trial = contract(
        fields.reshape(-1, chol), cholesky_vectors, trial_state, deviation[0]
    )
    steps, left = chain(packed, trial, electrons)
    square = jax.ShapeDtypeStruct((orbitals, orbitals), jnp.float32)
    density = call(
        functools.partial(green_kernel, 1.0 / (members * blocks)),
        square,
        (left, steps, walkers),
        [pltpu.VMEM((members, electrons, orbitals), jnp.float32)]
        + [pltpu.VMEM((members, electrons, electrons), jnp.float32)] * 3,
    )
    return spread(density)


def solution(mesh):
    sections, walks = mesh.devices.shape

    def run(fields, cholesky_vectors, trial_state, deviation):
        members = deviation.shape[1] // walks
        split_mesh = Mesh(
            mesh.devices.reshape(sections // members, members, walks),
            ("block", "member", "walk"),
        )
        section = ("block", "member")
        in_specs = (
            P(section, None, "walk"),
            P("walk", None, None),
            P(),
            P(section, "walk", None, None),
        )
        return jax.shard_map(
            body, mesh=split_mesh, in_specs=in_specs, out_specs=P("walk", None, None),
            check_vma=False,
        )(fields, cholesky_vectors, trial_state, deviation)

    return run
```

```python
import functools

import jax
import jax.numpy as jnp
from jax import lax
from jax.experimental import pallas as pl
from jax.experimental.pallas import tpu as pltpu
from jax.sharding import Mesh, PartitionSpec as P


SUB = 8
LANES = 128
DEPTH = 4
GROUP = 1
CHUNKS = 2
ROUGH_STEPS = 24
ROUGH_REST = 0.05
REST = 1e-5
START = 1.9
MESH = pl.DeviceIdType.MESH


def split(a):
    high = a.astype(jnp.bfloat16)
    return high, (a - high.astype(jnp.float32)).astype(jnp.bfloat16)


def dot_f32(a, b):
    return jnp.dot(a, b, preferred_element_type=jnp.float32)


def dot3(a, b):
    a_high, a_low = split(a)
    b_high, b_low = split(b)
    return dot_f32(a_high, b_high) + (dot_f32(a_high, b_low) + dot_f32(a_low, b_high))


def greet(peers):
    barrier = pltpu.get_barrier_semaphore()
    for peer in peers:
        pl.semaphore_signal(barrier, inc=1, device_id=peer, device_id_type=MESH)
    return barrier


def fold_rows(orbitals):
    return (orbitals // SUB + 1) // 2 * SUB


def contract_kernel(
    per, field_ref, table_ref, packed_ref, factor, low, high, part, gathered,
    low_sem, high_sem, v_send, v_recv,
):
    rows, chol = field_ref.shape
    orbitals = table_ref.shape[1]
    members, walks = lax.axis_size("member"), lax.axis_size("walk")
    member, walk = lax.axis_index("member"), lax.axis_index("walk")
    half = fold_rows(orbitals)
    bands, folds = orbitals // SUB, half // SUB
    depth = chol * SUB
    order = [band for f in range(folds) for band in (f, f + folds) if band < bands]

    def fetch(place):
        band, slot = order[place], place % DEPTH
        at = pl.ds(band * SUB, SUB)
        copies = [
            pltpu.make_async_copy(
                table_ref.at[:, at, pl.ds(LANES, orbitals - LANES)], high.at[slot], high_sem.at[slot]
            )
        ]
        if band * SUB < LANES:
            copies.append(
                pltpu.make_async_copy(
                    table_ref.at[:, at, pl.ds(0, LANES)], low.at[slot], low_sem.at[slot]
                )
            )
        return copies

    flight = {}

    def start(place):
        if place < len(order):
            flight[place] = fetch(place)
            for copy in flight[place]:
                copy.start()

    for place in range(DEPTH):
        start(place)
    owners = [
        {"walk": lax.rem(walk + i, walks), "member": lax.rem(member + j, members)}
        for i in range(walks)
        for j in range(members)
    ][1:]
    barrier = greet(owners)
    vector = lax.broadcasted_iota(jnp.int32, (chol, LANES), 0)
    lane = lax.broadcasted_iota(jnp.int32, (chol, LANES), 1)
    keep = lax.broadcasted_iota(jnp.int32, (2 * SUB, LANES), 0) % SUB
    keep = keep == lax.broadcasted_iota(jnp.int32, (2 * SUB, LANES), 1) % SUB
    for j in range(pl.cdiv(depth, LANES)):
        width = min(LANES, depth - j * LANES)
        pick = jnp.where(vector == j * (LANES // SUB) + lane // SUB, 1.0, 0.0)
        spread = dot_f32(field_ref[...], pick.astype(jnp.bfloat16))
        for row in range(0, rows, 2):
            pair = jnp.concatenate(
                [
                    jnp.broadcast_to(spread[row + i : row + i + 1], (SUB, LANES))
                    for i in range(2)
                ],
                axis=0,
            )
            factor[row * SUB : (row + 2) * SUB, j * LANES : j * LANES + width] = jnp.where(
                keep, pair, 0.0
            ).astype(jnp.bfloat16)[:, :width]

    def product(place):
        band, slot = order[place], place % DEPTH
        for copy in flight[place]:
            copy.wait()
        right = dot_f32(factor[...], high[slot].reshape(depth, orbitals - LANES))
        right = right.reshape(rows, SUB, orbitals - LANES)
        left = None
        if band * SUB < LANES:
            left = dot_f32(factor[...], low[slot].reshape(depth, LANES))
            left = left.reshape(rows, SUB, LANES)
        return left, right

    def v_copy(i, group):
        owner = owners[i]
        at = pl.ds(group[0] * SUB, len(group) * SUB)
        return pltpu.make_async_remote_copy(
            src_ref=part.at[owner["walk"] * per + owner["member"], at, :],
            dst_ref=gathered.at[walk, member, at, :],
            send_sem=v_send.at[i, group[0]],
            recv_sem=v_recv.at[i, group[0]],
            device_id=owner,
            device_id_type=MESH,
        )

    groups = [list(range(f, min(f + GROUP, folds))) for f in range(0, folds, GROUP)]
    sub = lax.broadcasted_iota(jnp.int32, (SUB, orbitals), 0)
    column = lax.broadcasted_iota(jnp.int32, (SUB, orbitals), 1)
    place = 0
    for f in range(folds + 1):
        if f < folds:
            left, right = product(place)
            start(place + DEPTH)
            place += 1
            upper = jnp.concatenate([left, right], axis=2)
            if f + folds < bands:
                left, right = product(place)
                start(place + DEPTH)
                place += 1
                if left is not None:
                    right = jnp.concatenate([left[:, :, half:], right], axis=2)
                    pad = 0
                else:
                    pad = LANES - half
                pieces = [right, jnp.zeros((rows, SUB, half), jnp.float32)]
                if pad:
                    pieces = [jnp.zeros((rows, SUB, pad), jnp.float32)] + pieces
                lower = jnp.concatenate(pieces, axis=2)
            else:
                lower = jnp.zeros_like(upper)
            own = (column >= half) | (column < f * SUB + sub)
            part[:, f * SUB : (f + 1) * SUB, :] = jnp.where(own[None], upper, lower)
        if f == 0:
            pl.semaphore_wait(barrier, len(owners))
        for group in groups:
            if group[-1] == f - 1:
                for i in range(len(owners)):
                    v_copy(i, group).start()
    gathered[walk, member] = part[walk * per + member]
    for group in groups:
        for i in range(len(owners)):
            v_copy(i, group).wait_recv()
    packed_ref[...] = sum(gathered[i] for i in range(1, walks)) + gathered[0]
    for group in groups:
        for i in range(len(owners)):
            v_copy(i, group).wait_send()


def contract(field_rows, cholesky_vectors, per):
    rows, chol = field_rows.shape
    orbitals = cholesky_vectors.shape[1]
    members, walks = lax.axis_size("member"), lax.axis_size("walk")
    half = fold_rows(orbitals)
    vmem = pl.BlockSpec(memory_space=pltpu.VMEM)
    f32, bf16, dma = jnp.float32, jnp.bfloat16, pltpu.SemaphoreType.DMA
    return pl.pallas_call(
        functools.partial(contract_kernel, per),
        in_specs=[vmem, pl.BlockSpec(memory_space=pl.ANY)],
        out_specs=vmem,
        out_shape=jax.ShapeDtypeStruct((members, half, orbitals), f32),
        scratch_shapes=[
            pltpu.VMEM((rows * SUB, chol * SUB), bf16),
            pltpu.VMEM((DEPTH, chol, SUB, LANES), bf16),
            pltpu.VMEM((DEPTH, chol, SUB, orbitals - LANES), bf16),
            pltpu.VMEM((rows, half, orbitals), f32),
            pltpu.VMEM((walks, members, half, orbitals), f32),
            dma((DEPTH,)),
            dma((DEPTH,)),
            dma((walks * members - 1, half // SUB)),
            dma((walks * members - 1, half // SUB)),
        ],
        compiler_params=pltpu.CompilerParams(
            vmem_limit_bytes=48 * 2**20, collective_id=0, has_side_effects=True
        ),
        cost_estimate=pl.CostEstimate(
            flops=2 * rows * SUB * SUB * chol * orbitals * orbitals,
            bytes_accessed=2 * chol * orbitals * orbitals,
            transcendentals=0,
        ),
    )(field_rows, cholesky_vectors)


def eye(size):
    row = lax.broadcasted_iota(jnp.int32, (size, size), 0)
    column = lax.broadcasted_iota(jnp.int32, (size, size), 1)
    return jnp.where(row == column, 1.0, 0.0)


def unfold(packed):
    half, orbitals = packed.shape
    rest = orbitals - half
    row = lax.broadcasted_iota(jnp.int32, (half, half), 0)
    column = lax.broadcasted_iota(jnp.int32, (half, half), 1)
    square = packed[:, :half]
    flipped = -square.T
    first = jnp.where(row > column, square, jnp.where(row < column, flipped, 0.0))
    second = jnp.where(row < column, square, jnp.where(row > column, flipped, 0.0))
    across = packed[:, half:]
    return jnp.concatenate(
        [
            jnp.concatenate([first, across], axis=1),
            jnp.concatenate([-across.T, second[:rest, :rest]], axis=1),
        ],
        axis=0,
    )


def series(v, unit):
    v2 = dot3(v, v)
    v3 = dot3(v2, v)
    upper = unit * (1 / 6) + v * (1 / 24) + v2 * (1 / 120) + v3 * (1 / 720)
    return (unit + v + v2 * 0.5) + dot3(v3, upper)


def chain_kernel(
    packed_ref, trial_ref, deviation_ref, maps_ref, cross_ref, left_ref, walkers_ref,
    steps, held, sent, walk_send, walk_recv, send_sem, recv_sem, w_send, w_recv,
):
    members = packed_ref.shape[0]
    padded, orbitals = held.shape
    electrons = trial_ref.shape[1]
    blocks, block = lax.axis_size("block"), lax.axis_index("block")
    member = lax.axis_index("member")
    has_next, has_last = block < blocks - 1, block > 0
    after, before = lax.rem(block + 1, blocks), lax.rem(block + blocks - 1, blocks)
    bands = padded // SUB
    cuts = [c * bands // CHUNKS * SUB for c in range(CHUNKS)] + [padded]
    others = [lax.rem(member + shift, members) for shift in range(1, members)]
    barrier = greet([{"member": other} for other in others])
    for near, peer in ((has_next, after), (has_last, before)):
        @pl.when(near)
        def _():
            pl.semaphore_signal(barrier, inc=1, device_id={"block": peer}, device_id_type=MESH)

    def w_copy(shift):
        return pltpu.make_async_remote_copy(
            src_ref=walk_send.at[others[shift - 1]],
            dst_ref=walk_recv.at[member],
            send_sem=w_send.at[shift - 1],
            recv_sem=w_recv.at[shift - 1],
            device_id={"member": others[shift - 1]},
            device_id_type=MESH,
        )

    def copy(i):
        at = pl.ds(cuts[i], cuts[i + 1] - cuts[i])
        return pltpu.make_async_remote_copy(
            src_ref=sent.at[at, :],
            dst_ref=held.at[at, :],
            send_sem=send_sem.at[i],
            recv_sem=recv_sem.at[i],
            device_id={"block": before},
            device_id_type=MESH,
        )

    walk_send[...] = trial_ref[...] + deviation_ref[...].astype(jnp.float32)
    unit = eye(orbitals)
    steps[members - 1] = series(unfold(packed_ref[members - 1]), unit)
    pl.semaphore_wait(
        barrier, has_next.astype(jnp.int32) + has_last.astype(jnp.int32) + len(others)
    )
    for shift in range(1, members):
        w_copy(shift).start()
    for s in range(members - 1):
        steps[s] = series(unfold(packed_ref[s]), unit)
    parts = [steps[s] for s in reversed(range(members))]
    while len(parts) > 1:
        paired = [dot3(parts[i], parts[i + 1]) for i in range(0, len(parts) - 1, 2)]
        parts = paired + parts[len(parts) - len(parts) % 2 :]
    maps_ref[0] = parts[0]

    def pass_on(i):
        at = slice(cuts[i], cuts[i + 1])
        sent[at, :] = dot3(held[at, :], maps_ref[0])
        copy(i).start()

    @pl.when(jnp.logical_not(has_next))
    def _():
        held[...] = jnp.zeros_like(held)
        held[:electrons, :] = trial_ref[...].T
        for i in range(CHUNKS):
            pass_on(i)

    maps_ref[members - 1] = steps[members - 1]
    for s in reversed(range(1, members - 1)):
        maps_ref[s] = dot3(maps_ref[s + 1], steps[s])
    walkers_ref[member] = walk_send[member]
    for shift in range(1, members):
        source = lax.rem(member + members - shift, members)
        w_copy(shift).wait()
        walkers_ref[source] = walk_recv[source]
    for s in range(members):
        cross_ref[s] = dot3(maps_ref[s], walkers_ref[s])

    @pl.when(has_next)
    def _():
        for i in range(CHUNKS):
            copy(i).wait_recv()

            @pl.when(has_last)
            def _():
                pass_on(i)

    left_ref[...] = held[:electrons, :]

    @pl.when(has_last)
    def _():
        for i in range(CHUNKS):
            copy(i).wait_send()


def chain(packed, trial_state, deviation):
    members = packed.shape[0]
    orbitals, electrons = trial_state.shape
    padded = -(-electrons // SUB) * SUB
    vmem, dma = pl.BlockSpec(memory_space=pltpu.VMEM), pltpu.SemaphoreType.DMA
    walkers = (members, orbitals, electrons)
    square = (members, orbitals, orbitals)
    return pl.pallas_call(
        chain_kernel,
        in_specs=[vmem] * 3,
        out_specs=[vmem] * 4,
        out_shape=[
            jax.ShapeDtypeStruct(shape, jnp.float32)
            for shape in (square, walkers, (electrons, orbitals), walkers)
        ],
        scratch_shapes=[
            pltpu.VMEM(shape, jnp.float32)
            for shape in (square, (padded, orbitals), (padded, orbitals), walkers, walkers)
        ]
        + [dma((CHUNKS,))] * 2
        + [dma((members - 1,))] * 2,
        compiler_params=pltpu.CompilerParams(
            vmem_limit_bytes=48 * 2**20, collective_id=1, has_side_effects=True
        ),
    )(packed, trial_state, deviation)


def green_kernel(
    scale, left_in_ref, maps_ref, cross_ref, walk_ref, out_ref, left_ref, inter_ref,
    inverse_ref, first_ref,
):
    members = maps_ref.shape[0]
    unit = eye(left_in_ref.shape[0])

    def rounded(a, b):
        return dot_f32(a.astype(jnp.bfloat16), b.astype(jnp.bfloat16))

    levels = []
    for s in range(members):
        inter = dot3(left_in_ref[...], cross_ref[s])
        levels.append(1.0 / jnp.max(jnp.abs(inter)))
        inter = inter * levels[s]
        inter_ref[s] = inter
        flipped = inter.T
        square = rounded(inter, flipped)
        square = rounded(square, square)
        first = flipped * (START * lax.rsqrt(lax.sqrt(jnp.sum(square * square))))
        inverse_ref[s] = first
        first_ref[s] = first
        left_ref[s] = dot3(left_in_ref[...], maps_ref[s])

    def newton(dot):
        worst = jnp.float32(0.0)
        for s in range(members):
            guess = inverse_ref[s]
            rest = unit - dot(inter_ref[s], guess)
            inverse_ref[s] = guess + dot(guess, rest)
            worst = jnp.maximum(worst, jnp.sum(rest * rest))
        return worst

    _, rough = lax.while_loop(
        lambda state: (state[0] < ROUGH_STEPS) & (state[1] > ROUGH_REST),
        lambda state: (state[0] + 1, newton(rounded)),
        (jnp.int32(0), jnp.float32(unit.shape[0])),
    )

    @pl.when(jnp.logical_not(rough <= ROUGH_REST))
    def _():
        for s in range(members):
            inverse_ref[s] = first_ref[s]

    lax.while_loop(
        lambda state: (state[0] < 80) & (state[1] > REST),
        lambda state: (state[0] + 1, newton(dot3)),
        (jnp.int32(0), jnp.float32(unit.shape[0])),
    )
    total = None
    for s in range(members):
        solved = dot3(inverse_ref[s], left_ref[s]) * (levels[s] * scale)
        green = dot3(walk_ref[s], solved)
        total = green if total is None else total + green
    out_ref[...] = total


def call(kernel, out_shape, args, scratch=(), scalars=0):
    vmem = pl.BlockSpec(memory_space=pltpu.VMEM)
    smem = pl.BlockSpec(memory_space=pltpu.SMEM)
    return pl.pallas_call(
        kernel,
        in_specs=[smem] * scalars + [vmem] * (len(args) - scalars),
        out_specs=vmem,
        out_shape=out_shape,
        scratch_shapes=list(scratch),
        compiler_params=pltpu.CompilerParams(vmem_limit_bytes=48 * 2**20),
    )(*args)


def spread_kernel(density_ref, out_ref, mine, arrived, whole, *sems):
    sum_send, sum_recv, all_send, all_recv, near_send, near_recv = sems
    orbitals = density_ref.shape[0]
    blocks, piece, _ = mine.shape
    members = whole.shape[0]
    block, member = lax.axis_index("block"), lax.axis_index("member")
    bits = [1 << i for i in reversed(range(members.bit_length() - 1))]
    offsets, pairs = [0], []
    for bit in bits:
        pairs += [(bit, offset) for offset in offsets]
        offsets += [offset + bit for offset in offsets]
    came = {bit + offset: j for j, (bit, offset) in enumerate(pairs)}
    shifts = sorted(range(1, blocks), key=lambda shift: min(shift, blocks - shift))

    def flip(offset):
        place = member
        for bit in bits:
            if offset & bit:
                place = place + bit - 2 * bit * ((place // bit) % 2)
        return place

    def remote(source, target, send, recv, device):
        return pltpu.make_async_remote_copy(
            src_ref=source, dst_ref=target, send_sem=send, recv_sem=recv,
            device_id=device, device_id_type=MESH,
        )

    def to_sum(shift):
        peer = lax.rem(block + shift, blocks)
        return remote(
            mine.at[peer], arrived.at[shift - 1],
            sum_send.at[shift - 1], sum_recv.at[shift - 1], {"block": peer},
        )

    def to_all(shift):
        ref = whole.at[member, block]
        return remote(
            ref, ref, all_send.at[shift - 1], all_recv.at[shift - 1],
            {"block": lax.rem(block + shift, blocks)},
        )

    def near(j, shift):
        bit, offset = pairs[j]
        ref = whole.at[flip(offset), lax.rem(block + blocks - shift, blocks)]
        return remote(
            ref, ref, near_send.at[j, shift], near_recv.at[j, shift], {"member": flip(bit)}
        )

    barrier = greet(
        [{"block": lax.rem(block + shift, blocks)} for shift in shifts]
        + [{"member": flip(bit)} for bit in bits]
    )
    for q in range(blocks):
        rows = min(piece, orbitals - q * piece)
        if rows > 0:
            mine[q, :rows, :] = density_ref[q * piece : q * piece + rows, :]
        if rows < piece:
            mine[q, max(rows, 0) :, :] = jnp.zeros((piece - max(rows, 0), orbitals), jnp.float32)
    pl.semaphore_wait(barrier, len(shifts) + len(bits))
    for shift in shifts:
        to_sum(shift).start()
    value = mine[block]
    for shift in shifts:
        to_sum(shift).wait_recv()
        value = value + arrived[shift - 1]
    whole[member, block] = value
    for shift in shifts:
        to_all(shift).start()
    for shift in [0] + shifts:
        if shift:
            to_all(shift).wait_recv()
        for j, (bit, offset) in enumerate(pairs):
            if not offset:
                near(j, shift).start()
    waited = set()
    for offset in offsets[1:]:
        for shift in [0] + shifts:
            for j, (bit, held) in enumerate(pairs):
                if held == offset:
                    if (came[offset], shift) not in waited:
                        near(came[offset], shift).wait_recv()
                        waited.add((came[offset], shift))
                    near(j, shift).start()
    for shift in [0] + shifts:
        for j in range(len(pairs)):
            if (j, shift) not in waited:
                near(j, shift).wait_recv()
    for q in range(blocks):
        rows = min(piece, orbitals - q * piece)
        if rows > 0:
            out_ref[:, q * piece : q * piece + rows, :] = whole[:, q, :rows, :]
    for shift in [0] + shifts:
        if shift:
            to_sum(shift).wait_send()
            to_all(shift).wait_send()
        for j in range(len(pairs)):
            near(j, shift).wait_send()


def spread(density):
    blocks, members = lax.axis_size("block"), lax.axis_size("member")
    if members & (members - 1):
        return lax.all_gather(lax.psum(density, "block"), "member")
    orbitals = density.shape[0]
    piece = pl.cdiv(pl.cdiv(orbitals, SUB), blocks) * SUB
    vmem, dma = pl.BlockSpec(memory_space=pltpu.VMEM), pltpu.SemaphoreType.DMA
    return pl.pallas_call(
        spread_kernel,
        in_specs=[vmem],
        out_specs=vmem,
        out_shape=jax.ShapeDtypeStruct((members, orbitals, orbitals), jnp.float32),
        scratch_shapes=[
            pltpu.VMEM((blocks, piece, orbitals), jnp.float32),
            pltpu.VMEM((blocks - 1, piece, orbitals), jnp.float32),
            pltpu.VMEM((members, blocks, piece, orbitals), jnp.float32),
        ]
        + [dma((blocks - 1,))] * 4
        + [dma((members - 1, blocks))] * 2,
        compiler_params=pltpu.CompilerParams(
            vmem_limit_bytes=48 * 2**20, collective_id=2, has_side_effects=True
        ),
    )(density)


def body(fields, cholesky_vectors, trial_state, deviation):
    chol = fields.shape[2]
    orbitals, electrons = trial_state.shape
    blocks, members = lax.axis_size("block"), lax.axis_size("member")
    packed = contract(fields.reshape(-1, chol), cholesky_vectors, deviation.shape[1])
    maps, cross, left, walkers = chain(packed, trial_state, deviation[0])
    square = jax.ShapeDtypeStruct((orbitals, orbitals), jnp.float32)
    density = call(
        functools.partial(green_kernel, 1.0 / (members * blocks)),
        square,
        (left, maps, cross, walkers),
        [pltpu.VMEM((members, electrons, orbitals), jnp.float32)]
        + [pltpu.VMEM((members, electrons, electrons), jnp.float32)] * 3,
    )
    return spread(density)


def solution(mesh):
    sections, walks = mesh.devices.shape

    def run(fields, cholesky_vectors, trial_state, deviation):
        members = deviation.shape[1] // walks
        split_mesh = Mesh(
            mesh.devices.reshape(sections // members, members, walks),
            ("block", "member", "walk"),
        )
        section = ("block", "member")
        in_specs = (
            P(section, None, "walk"),
            P("walk", None, None),
            P(),
            P(section, "walk", None, None),
        )
        return jax.shard_map(
            body, mesh=split_mesh, in_specs=in_specs, out_specs=P("walk", None, None),
            check_vma=False,
        )(fields, cholesky_vectors, trial_state, deviation)

    return run
```

```python
import functools

import jax
import jax.numpy as jnp
from jax import lax
from jax.experimental import pallas as pl
from jax.experimental.pallas import tpu as pltpu
from jax.sharding import Mesh, PartitionSpec as P


SUB = 8
LANES = 128
DEPTH = 4
GROUP = 1
CHUNKS = 3
ROUGH_STEPS = 8
ROUGH_REST = 0.2
REST = 4e-5
START = 1.9
MESH = pl.DeviceIdType.MESH


def split(a):
    high = a.astype(jnp.bfloat16)
    return high, (a - high.astype(jnp.float32)).astype(jnp.bfloat16)


def dot_f32(a, b):
    return jnp.dot(a, b, preferred_element_type=jnp.float32)


def dot3(a, b):
    a_high, a_low = split(a)
    b_high, b_low = split(b)
    return dot_f32(a_high, b_high) + (dot_f32(a_high, b_low) + dot_f32(a_low, b_high))


def greet(peers):
    barrier = pltpu.get_barrier_semaphore()
    for peer in peers:
        pl.semaphore_signal(barrier, inc=1, device_id=peer, device_id_type=MESH)
    return barrier


def fold_rows(orbitals):
    return (orbitals // SUB + 1) // 2 * SUB


def contract_kernel(
    per, field_ref, table_ref, packed_ref, factor, low, high, part, gathered,
    low_sem, high_sem, v_send, v_recv,
):
    rows, chol = field_ref.shape
    orbitals = table_ref.shape[1]
    members, walks = lax.axis_size("member"), lax.axis_size("walk")
    member, walk = lax.axis_index("member"), lax.axis_index("walk")
    half = fold_rows(orbitals)
    bands, folds = orbitals // SUB, half // SUB
    depth = chol * SUB
    order = [band for f in range(folds) for band in (f, f + folds) if band < bands]

    def fetch(place):
        band, slot = order[place], place % DEPTH
        at = pl.ds(band * SUB, SUB)
        copies = [
            pltpu.make_async_copy(
                table_ref.at[:, at, pl.ds(LANES, orbitals - LANES)], high.at[slot], high_sem.at[slot]
            )
        ]
        if band * SUB < LANES:
            copies.append(
                pltpu.make_async_copy(
                    table_ref.at[:, at, pl.ds(0, LANES)], low.at[slot], low_sem.at[slot]
                )
            )
        return copies

    flight = {}

    def start(place):
        if place < len(order):
            flight[place] = fetch(place)
            for copy in flight[place]:
                copy.start()

    for place in range(DEPTH):
        start(place)
    owners = [
        {"walk": lax.rem(walk + i, walks), "member": lax.rem(member + j, members)}
        for i in range(walks)
        for j in range(members)
    ][1:]
    barrier = greet(owners)
    vector = lax.broadcasted_iota(jnp.int32, (chol, LANES), 0)
    lane = lax.broadcasted_iota(jnp.int32, (chol, LANES), 1)
    keep = lax.broadcasted_iota(jnp.int32, (2 * SUB, LANES), 0) % SUB
    keep = keep == lax.broadcasted_iota(jnp.int32, (2 * SUB, LANES), 1) % SUB
    for j in range(pl.cdiv(depth, LANES)):
        width = min(LANES, depth - j * LANES)
        pick = jnp.where(vector == j * (LANES // SUB) + lane // SUB, 1.0, 0.0)
        spread = dot_f32(field_ref[...], pick.astype(jnp.bfloat16))
        for row in range(0, rows, 2):
            pair = jnp.concatenate(
                [
                    jnp.broadcast_to(spread[row + i : row + i + 1], (SUB, LANES))
                    for i in range(2)
                ],
                axis=0,
            )
            factor[row * SUB : (row + 2) * SUB, j * LANES : j * LANES + width] = jnp.where(
                keep, pair, 0.0
            ).astype(jnp.bfloat16)[:, :width]

    def product(place):
        band, slot = order[place], place % DEPTH
        for copy in flight[place]:
            copy.wait()
        right = dot_f32(factor[...], high[slot].reshape(depth, orbitals - LANES))
        right = right.reshape(rows, SUB, orbitals - LANES)
        left = None
        if band * SUB < LANES:
            left = dot_f32(factor[...], low[slot].reshape(depth, LANES))
            left = left.reshape(rows, SUB, LANES)
        return left, right

    def v_copy(i, group):
        owner = owners[i]
        at = pl.ds(group[0] * SUB, len(group) * SUB)
        return pltpu.make_async_remote_copy(
            src_ref=part.at[owner["walk"] * per + owner["member"], at, :],
            dst_ref=gathered.at[walk, member, at, :],
            send_sem=v_send.at[i, group[0]],
            recv_sem=v_recv.at[i, group[0]],
            device_id=owner,
            device_id_type=MESH,
        )

    groups = [list(range(f, min(f + GROUP, folds))) for f in range(0, folds, GROUP)]
    sub = lax.broadcasted_iota(jnp.int32, (SUB, orbitals), 0)
    column = lax.broadcasted_iota(jnp.int32, (SUB, orbitals), 1)
    place = 0
    for f in range(folds + 1):
        if f < folds:
            left, right = product(place)
            start(place + DEPTH)
            place += 1
            upper = jnp.concatenate([left, right], axis=2)
            if f + folds < bands:
                left, right = product(place)
                start(place + DEPTH)
                place += 1
                if left is not None:
                    right = jnp.concatenate([left[:, :, half:], right], axis=2)
                    pad = 0
                else:
                    pad = LANES - half
                pieces = [right, jnp.zeros((rows, SUB, half), jnp.float32)]
                if pad:
                    pieces = [jnp.zeros((rows, SUB, pad), jnp.float32)] + pieces
                lower = jnp.concatenate(pieces, axis=2)
            else:
                lower = jnp.zeros_like(upper)
            own = (column >= half) | (column < f * SUB + sub)
            part[:, f * SUB : (f + 1) * SUB, :] = jnp.where(own[None], upper, lower)
        if f == 0:
            pl.semaphore_wait(barrier, len(owners))
        for group in groups:
            if group[-1] == f - 1:
                for i in range(len(owners)):
                    v_copy(i, group).start()
    gathered[walk, member] = part[walk * per + member]
    for group in groups:
        for i in range(len(owners)):
            v_copy(i, group).wait_recv()
    packed_ref[...] = sum(gathered[i] for i in range(1, walks)) + gathered[0]
    for group in groups:
        for i in range(len(owners)):
            v_copy(i, group).wait_send()


def contract(field_rows, cholesky_vectors, per):
    rows, chol = field_rows.shape
    orbitals = cholesky_vectors.shape[1]
    members, walks = lax.axis_size("member"), lax.axis_size("walk")
    half = fold_rows(orbitals)
    vmem = pl.BlockSpec(memory_space=pltpu.VMEM)
    f32, bf16, dma = jnp.float32, jnp.bfloat16, pltpu.SemaphoreType.DMA
    return pl.pallas_call(
        functools.partial(contract_kernel, per),
        in_specs=[vmem, pl.BlockSpec(memory_space=pl.ANY)],
        out_specs=vmem,
        out_shape=jax.ShapeDtypeStruct((members, half, orbitals), f32),
        scratch_shapes=[
            pltpu.VMEM((rows * SUB, chol * SUB), bf16),
            pltpu.VMEM((DEPTH, chol, SUB, LANES), bf16),
            pltpu.VMEM((DEPTH, chol, SUB, orbitals - LANES), bf16),
            pltpu.VMEM((rows, half, orbitals), f32),
            pltpu.VMEM((walks, members, half, orbitals), f32),
            dma((DEPTH,)),
            dma((DEPTH,)),
            dma((walks * members - 1, half // SUB)),
            dma((walks * members - 1, half // SUB)),
        ],
        compiler_params=pltpu.CompilerParams(
            vmem_limit_bytes=48 * 2**20, collective_id=0, has_side_effects=True
        ),
        cost_estimate=pl.CostEstimate(
            flops=2 * rows * SUB * SUB * chol * orbitals * orbitals,
            bytes_accessed=2 * chol * orbitals * orbitals,
            transcendentals=0,
        ),
    )(field_rows, cholesky_vectors)


def eye(size):
    row = lax.broadcasted_iota(jnp.int32, (size, size), 0)
    column = lax.broadcasted_iota(jnp.int32, (size, size), 1)
    return jnp.where(row == column, 1.0, 0.0)


def unfold(packed):
    half, orbitals = packed.shape
    rest = orbitals - half
    row = lax.broadcasted_iota(jnp.int32, (half, half), 0)
    column = lax.broadcasted_iota(jnp.int32, (half, half), 1)
    square = packed[:, :half]
    flipped = -square.T
    first = jnp.where(row > column, square, jnp.where(row < column, flipped, 0.0))
    second = jnp.where(row < column, square, jnp.where(row > column, flipped, 0.0))
    across = packed[:, half:]
    return jnp.concatenate(
        [
            jnp.concatenate([first, across], axis=1),
            jnp.concatenate([-across.T, second[:rest, :rest]], axis=1),
        ],
        axis=0,
    )


def series(v, unit):
    v2 = dot3(v, v)
    v3 = dot3(v2, v)
    upper = unit * (1 / 6) + v * (1 / 24) + v2 * (1 / 120) + v3 * (1 / 720)
    return (unit + v + v2 * 0.5) + dot3(v3, upper)


def chain_kernel(
    packed_ref, trial_ref, deviation_ref, maps_ref, cross_ref, left_ref, walkers_ref,
    steps, held, sent, walk_send, walk_recv, send_sem, recv_sem, w_send, w_recv,
):
    members = packed_ref.shape[0]
    padded, orbitals = held.shape
    electrons = trial_ref.shape[1]
    blocks, block = lax.axis_size("block"), lax.axis_index("block")
    member = lax.axis_index("member")
    has_next, has_last = block < blocks - 1, block > 0
    after, before = lax.rem(block + 1, blocks), lax.rem(block + blocks - 1, blocks)
    bands = padded // SUB
    cuts = [c * bands // CHUNKS * SUB for c in range(CHUNKS)] + [padded]
    others = [lax.rem(member + shift, members) for shift in range(1, members)]
    barrier = greet([{"member": other} for other in others])
    for near, peer in ((has_next, after), (has_last, before)):
        @pl.when(near)
        def _():
            pl.semaphore_signal(barrier, inc=1, device_id={"block": peer}, device_id_type=MESH)

    def w_copy(shift):
        return pltpu.make_async_remote_copy(
            src_ref=walk_send.at[others[shift - 1]],
            dst_ref=walk_recv.at[member],
            send_sem=w_send.at[shift - 1],
            recv_sem=w_recv.at[shift - 1],
            device_id={"member": others[shift - 1]},
            device_id_type=MESH,
        )

    def copy(i):
        at = pl.ds(cuts[i], cuts[i + 1] - cuts[i])
        return pltpu.make_async_remote_copy(
            src_ref=sent.at[at, :],
            dst_ref=held.at[at, :],
            send_sem=send_sem.at[i],
            recv_sem=recv_sem.at[i],
            device_id={"block": before},
            device_id_type=MESH,
        )

    walk_send[...] = trial_ref[...] + deviation_ref[...].astype(jnp.float32)
    unit = eye(orbitals)
    steps[members - 1] = series(unfold(packed_ref[members - 1]), unit)
    pl.semaphore_wait(
        barrier, has_next.astype(jnp.int32) + has_last.astype(jnp.int32) + len(others)
    )
    for shift in range(1, members):
        w_copy(shift).start()
    for s in range(members - 1):
        steps[s] = series(unfold(packed_ref[s]), unit)
    parts = [steps[s] for s in reversed(range(members))]
    while len(parts) > 1:
        paired = [dot3(parts[i], parts[i + 1]) for i in range(0, len(parts) - 1, 2)]
        parts = paired + parts[len(parts) - len(parts) % 2 :]
    maps_ref[0] = parts[0]

    def pass_on(i):
        at = slice(cuts[i], cuts[i + 1])
        sent[at, :] = dot3(held[at, :], maps_ref[0])
        copy(i).start()

    @pl.when(jnp.logical_not(has_next))
    def _():
        held[...] = jnp.zeros_like(held)
        held[:electrons, :] = trial_ref[...].T
        for i in range(CHUNKS):
            pass_on(i)

    maps_ref[members - 1] = steps[members - 1]
    for s in reversed(range(1, members - 1)):
        maps_ref[s] = dot3(maps_ref[s + 1], steps[s])
    @pl.when(has_next & has_last)
    def _():
        for i in range(CHUNKS):
            copy(i).wait_recv()
            pass_on(i)

    walkers_ref[member] = walk_send[member]
    for shift in range(1, members):
        source = lax.rem(member + members - shift, members)
        w_copy(shift).wait()
        walkers_ref[source] = walk_recv[source]
    for s in range(members):
        cross_ref[s] = dot3(maps_ref[s], walkers_ref[s])

    @pl.when(jnp.logical_not(has_last) & has_next)
    def _():
        for i in range(CHUNKS):
            copy(i).wait_recv()

    left_ref[...] = held[:electrons, :]

    @pl.when(has_last)
    def _():
        for i in range(CHUNKS):
            copy(i).wait_send()


def chain(packed, trial_state, deviation):
    members = packed.shape[0]
    orbitals, electrons = trial_state.shape
    padded = -(-electrons // SUB) * SUB
    vmem, dma = pl.BlockSpec(memory_space=pltpu.VMEM), pltpu.SemaphoreType.DMA
    walkers = (members, orbitals, electrons)
    square = (members, orbitals, orbitals)
    return pl.pallas_call(
        chain_kernel,
        in_specs=[vmem] * 3,
        out_specs=[vmem] * 4,
        out_shape=[
            jax.ShapeDtypeStruct(shape, jnp.float32)
            for shape in (square, walkers, (electrons, orbitals), walkers)
        ],
        scratch_shapes=[
            pltpu.VMEM(shape, jnp.float32)
            for shape in (square, (padded, orbitals), (padded, orbitals), walkers, walkers)
        ]
        + [dma((CHUNKS,))] * 2
        + [dma((members - 1,))] * 2,
        compiler_params=pltpu.CompilerParams(
            vmem_limit_bytes=48 * 2**20, collective_id=1, has_side_effects=True
        ),
    )(packed, trial_state, deviation)


def green_kernel(
    scale, left_in_ref, maps_ref, cross_ref, walk_ref, out_ref, left_ref, inter_ref,
    inverse_ref, first_ref,
):
    members = maps_ref.shape[0]
    unit = eye(left_in_ref.shape[0])

    def rounded(a, b):
        return dot_f32(a.astype(jnp.bfloat16), b.astype(jnp.bfloat16))

    levels = []
    for s in range(members):
        inter = dot3(left_in_ref[...], cross_ref[s])
        levels.append(1.0 / jnp.max(jnp.abs(inter), keepdims=True))
        inter_ref[s] = inter * levels[s]
    for s in range(members):
        inter = inter_ref[s]
        flipped = inter.T
        square = rounded(inter, flipped)
        square = rounded(square, square)
        size = jnp.sum(square * square, keepdims=True)
        first = flipped * (START * lax.rsqrt(lax.sqrt(size)))
        inverse_ref[s] = first
        first_ref[s] = first
        left_ref[s] = dot3(left_in_ref[...], maps_ref[s])

    def newton(dot):
        guesses = [inverse_ref[s] for s in range(members)]
        rests = [unit - dot(inter_ref[s], guesses[s]) for s in range(members)]
        for s in range(members):
            inverse_ref[s] = guesses[s] + dot(guesses[s], rests[s])
        return jnp.sum(sum(rest * rest for rest in rests[1:]) + rests[0] * rests[0])

    def rough_round():
        each = range(members)
        guesses = [inverse_ref[s] for s in each]
        powers = [unit - rounded(inter_ref[s], guesses[s]) for s in each]
        for _ in range(2):
            nexts = [rounded(powers[s], powers[s]) for s in each]
            guesses = [guesses[s] + rounded(guesses[s], powers[s]) for s in each]
            powers = nexts
        for s in each:
            inverse_ref[s] = guesses[s] + rounded(guesses[s], powers[s])
        return jnp.sum(sum(power * power for power in powers[1:]) + powers[0] * powers[0])

    def exact(most):
        return lax.while_loop(
            lambda state: (state[0] < most) & (state[1] > REST),
            lambda state: (state[0] + 1, newton(dot3)),
            (jnp.int32(0), jnp.float32(1.0)),
        )[1]

    lax.while_loop(
        lambda state: (state[0] < ROUGH_STEPS) & (state[1] > ROUGH_REST),
        lambda state: (state[0] + 1, rough_round()),
        (jnp.int32(0), jnp.float32(1.0)),
    )
    rest = exact(12)

    @pl.when(jnp.logical_not(rest <= REST))
    def _():
        for s in range(members):
            inverse_ref[s] = first_ref[s]
        exact(80)

    total = None
    for s in range(members):
        solved = dot3(inverse_ref[s], left_ref[s]) * (levels[s] * scale)
        green = dot3(walk_ref[s], solved)
        total = green if total is None else total + green
    out_ref[...] = total


def call(kernel, out_shape, args, scratch=(), scalars=0):
    vmem = pl.BlockSpec(memory_space=pltpu.VMEM)
    smem = pl.BlockSpec(memory_space=pltpu.SMEM)
    return pl.pallas_call(
        kernel,
        in_specs=[smem] * scalars + [vmem] * (len(args) - scalars),
        out_specs=vmem,
        out_shape=out_shape,
        scratch_shapes=list(scratch),
        compiler_params=pltpu.CompilerParams(vmem_limit_bytes=48 * 2**20),
    )(*args)


def spread_kernel(density_ref, out_ref, mine, arrived, whole, *sems):
    sum_send, sum_recv, all_send, all_recv, near_send, near_recv = sems
    orbitals = density_ref.shape[0]
    blocks, piece, _ = mine.shape
    members = whole.shape[0]
    block, member = lax.axis_index("block"), lax.axis_index("member")
    bits = [1 << i for i in reversed(range(members.bit_length() - 1))]
    offsets, pairs = [0], []
    for bit in bits:
        pairs += [(bit, offset) for offset in offsets]
        offsets += [offset + bit for offset in offsets]
    came = {bit + offset: j for j, (bit, offset) in enumerate(pairs)}
    shifts = sorted(range(1, blocks), key=lambda shift: min(shift, blocks - shift))

    def flip(offset):
        place = member
        for bit in bits:
            if offset & bit:
                place = place + bit - 2 * bit * ((place // bit) % 2)
        return place

    def remote(source, target, send, recv, device):
        return pltpu.make_async_remote_copy(
            src_ref=source, dst_ref=target, send_sem=send, recv_sem=recv,
            device_id=device, device_id_type=MESH,
        )

    def to_sum(shift):
        peer = lax.rem(block + shift, blocks)
        return remote(
            mine.at[peer], arrived.at[shift - 1],
            sum_send.at[shift - 1], sum_recv.at[shift - 1], {"block": peer},
        )

    def to_all(shift):
        ref = whole.at[member, block]
        return remote(
            ref, ref, all_send.at[shift - 1], all_recv.at[shift - 1],
            {"block": lax.rem(block + shift, blocks)},
        )

    def near(j, shift):
        bit, offset = pairs[j]
        ref = whole.at[flip(offset), lax.rem(block + blocks - shift, blocks)]
        return remote(
            ref, ref, near_send.at[j, shift], near_recv.at[j, shift], {"member": flip(bit)}
        )

    barrier = greet(
        [{"block": lax.rem(block + shift, blocks)} for shift in shifts]
        + [{"member": flip(bit)} for bit in bits]
    )
    for q in range(blocks):
        rows = min(piece, orbitals - q * piece)
        if rows > 0:
            mine[q, :rows, :] = density_ref[q * piece : q * piece + rows, :]
        if rows < piece:
            mine[q, max(rows, 0) :, :] = jnp.zeros((piece - max(rows, 0), orbitals), jnp.float32)
    pl.semaphore_wait(barrier, len(shifts) + len(bits))
    for shift in shifts:
        to_sum(shift).start()
    value = mine[block]
    for shift in shifts:
        to_sum(shift).wait_recv()
        value = value + arrived[shift - 1]
    whole[member, block] = value
    for shift in shifts:
        to_all(shift).start()
    for shift in [0] + shifts:
        if shift:
            to_all(shift).wait_recv()
        for j, (bit, offset) in enumerate(pairs):
            if not offset:
                near(j, shift).start()
    waited = set()
    for offset in offsets[1:]:
        for shift in [0] + shifts:
            for j, (bit, held) in enumerate(pairs):
                if held == offset:
                    if (came[offset], shift) not in waited:
                        near(came[offset], shift).wait_recv()
                        waited.add((came[offset], shift))
                    near(j, shift).start()
    for shift in [0] + shifts:
        for j in range(len(pairs)):
            if (j, shift) not in waited:
                near(j, shift).wait_recv()
    for q in range(blocks):
        rows = min(piece, orbitals - q * piece)
        if rows > 0:
            out_ref[:, q * piece : q * piece + rows, :] = whole[:, q, :rows, :]
    for shift in [0] + shifts:
        if shift:
            to_sum(shift).wait_send()
            to_all(shift).wait_send()
        for j in range(len(pairs)):
            near(j, shift).wait_send()


def spread(density):
    blocks, members = lax.axis_size("block"), lax.axis_size("member")
    if members & (members - 1):
        return lax.all_gather(lax.psum(density, "block"), "member")
    orbitals = density.shape[0]
    piece = pl.cdiv(pl.cdiv(orbitals, SUB), blocks) * SUB
    vmem, dma = pl.BlockSpec(memory_space=pltpu.VMEM), pltpu.SemaphoreType.DMA
    return pl.pallas_call(
        spread_kernel,
        in_specs=[vmem],
        out_specs=vmem,
        out_shape=jax.ShapeDtypeStruct((members, orbitals, orbitals), jnp.float32),
        scratch_shapes=[
            pltpu.VMEM((blocks, piece, orbitals), jnp.float32),
            pltpu.VMEM((blocks - 1, piece, orbitals), jnp.float32),
            pltpu.VMEM((members, blocks, piece, orbitals), jnp.float32),
        ]
        + [dma((blocks - 1,))] * 4
        + [dma((members - 1, blocks))] * 2,
        compiler_params=pltpu.CompilerParams(
            vmem_limit_bytes=48 * 2**20, collective_id=2, has_side_effects=True
        ),
    )(density)


def body(fields, cholesky_vectors, trial_state, deviation):
    chol = fields.shape[2]
    orbitals, electrons = trial_state.shape
    blocks, members = lax.axis_size("block"), lax.axis_size("member")
    packed = contract(fields.reshape(-1, chol), cholesky_vectors, deviation.shape[1])
    maps, cross, left, walkers = chain(packed, trial_state, deviation[0])
    square = jax.ShapeDtypeStruct((orbitals, orbitals), jnp.float32)
    density = call(
        functools.partial(green_kernel, 1.0 / (members * blocks)),
        square,
        (left, maps, cross, walkers),
        [pltpu.VMEM((members, electrons, orbitals), jnp.float32)]
        + [pltpu.VMEM((members, electrons, electrons), jnp.float32)] * 3,
    )
    return spread(density)


def solution(mesh):
    sections, walks = mesh.devices.shape

    def run(fields, cholesky_vectors, trial_state, deviation):
        members = deviation.shape[1] // walks
        split_mesh = Mesh(
            mesh.devices.reshape(sections // members, members, walks),
            ("block", "member", "walk"),
        )
        section = ("block", "member")
        in_specs = (
            P(section, None, "walk"),
            P("walk", None, None),
            P(),
            P(section, "walk", None, None),
        )
        return jax.shard_map(
            body, mesh=split_mesh, in_specs=in_specs, out_specs=P("walk", None, None),
            check_vma=False,
        )(fields, cholesky_vectors, trial_state, deviation)

    return run
```

```python
import functools

import jax
import jax.numpy as jnp
from jax import lax
from jax.experimental import pallas as pl
from jax.experimental.pallas import tpu as pltpu
from jax.sharding import Mesh, PartitionSpec as P


SUB = 8
LANES = 128
DEPTH = 4
GROUP = 1
CHUNKS = 4
ROUGH_STEPS = 8
ROUGH_REST = 0.2
REST = 4e-5
START = 1.9
MESH = pl.DeviceIdType.MESH


def split(a):
    high = a.astype(jnp.bfloat16)
    return high, (a - high.astype(jnp.float32)).astype(jnp.bfloat16)


def dot_f32(a, b):
    return jnp.dot(a, b, preferred_element_type=jnp.float32)


def dot3(a, b):
    a_high, a_low = split(a)
    b_high, b_low = split(b)
    return dot_f32(a_high, b_high) + (dot_f32(a_high, b_low) + dot_f32(a_low, b_high))


def greet(peers):
    barrier = pltpu.get_barrier_semaphore()
    for peer in peers:
        pl.semaphore_signal(barrier, inc=1, device_id=peer, device_id_type=MESH)
    return barrier


def fold_rows(orbitals):
    return (orbitals // SUB + 1) // 2 * SUB


def contract_kernel(
    per, field_ref, table_ref, packed_ref, factor, low, high, part, gathered,
    low_sem, high_sem, v_send, v_recv,
):
    rows, chol = field_ref.shape
    orbitals = table_ref.shape[1]
    members, walks = lax.axis_size("member"), lax.axis_size("walk")
    member, walk = lax.axis_index("member"), lax.axis_index("walk")
    half = fold_rows(orbitals)
    bands, folds = orbitals // SUB, half // SUB
    depth = chol * SUB
    order = [band for f in range(folds) for band in (f, f + folds) if band < bands]

    def fetch(place):
        band, slot = order[place], place % DEPTH
        at = pl.ds(band * SUB, SUB)
        copies = [
            pltpu.make_async_copy(
                table_ref.at[:, at, pl.ds(LANES, orbitals - LANES)], high.at[slot], high_sem.at[slot]
            )
        ]
        if band * SUB < LANES:
            copies.append(
                pltpu.make_async_copy(
                    table_ref.at[:, at, pl.ds(0, LANES)], low.at[slot], low_sem.at[slot]
                )
            )
        return copies

    flight = {}

    def start(place):
        if place < len(order):
            flight[place] = fetch(place)
            for copy in flight[place]:
                copy.start()

    for place in range(DEPTH):
        start(place)
    owners = [
        {"walk": lax.rem(walk + i, walks), "member": lax.rem(member + j, members)}
        for i in range(walks)
        for j in range(members)
    ][1:]
    barrier = greet(owners)
    vector = lax.broadcasted_iota(jnp.int32, (chol, LANES), 0)
    lane = lax.broadcasted_iota(jnp.int32, (chol, LANES), 1)
    keep = lax.broadcasted_iota(jnp.int32, (2 * SUB, LANES), 0) % SUB
    keep = keep == lax.broadcasted_iota(jnp.int32, (2 * SUB, LANES), 1) % SUB
    for j in range(pl.cdiv(depth, LANES)):
        width = min(LANES, depth - j * LANES)
        pick = jnp.where(vector == j * (LANES // SUB) + lane // SUB, 1.0, 0.0)
        spread = dot_f32(field_ref[...], pick.astype(jnp.bfloat16))
        for row in range(0, rows, 2):
            pair = jnp.concatenate(
                [
                    jnp.broadcast_to(spread[row + i : row + i + 1], (SUB, LANES))
                    for i in range(2)
                ],
                axis=0,
            )
            factor[row * SUB : (row + 2) * SUB, j * LANES : j * LANES + width] = jnp.where(
                keep, pair, 0.0
            ).astype(jnp.bfloat16)[:, :width]

    def product(place):
        band, slot = order[place], place % DEPTH
        for copy in flight[place]:
            copy.wait()
        right = dot_f32(factor[...], high[slot].reshape(depth, orbitals - LANES))
        right = right.reshape(rows, SUB, orbitals - LANES)
        left = None
        if band * SUB < LANES:
            left = dot_f32(factor[...], low[slot].reshape(depth, LANES))
            left = left.reshape(rows, SUB, LANES)
        return left, right

    def v_copy(i, group):
        owner = owners[i]
        at = pl.ds(group[0] * SUB, len(group) * SUB)
        return pltpu.make_async_remote_copy(
            src_ref=part.at[owner["walk"] * per + owner["member"], at, :],
            dst_ref=gathered.at[walk, member, at, :],
            send_sem=v_send.at[i, group[0]],
            recv_sem=v_recv.at[i, group[0]],
            device_id=owner,
            device_id_type=MESH,
        )

    groups = [list(range(f, min(f + GROUP, folds))) for f in range(0, folds, GROUP)]
    sub = lax.broadcasted_iota(jnp.int32, (SUB, orbitals), 0)
    column = lax.broadcasted_iota(jnp.int32, (SUB, orbitals), 1)
    place = 0
    for f in range(folds + 1):
        if f < folds:
            left, right = product(place)
            start(place + DEPTH)
            place += 1
            upper = jnp.concatenate([left, right], axis=2)
            if f + folds < bands:
                left, right = product(place)
                start(place + DEPTH)
                place += 1
                if left is not None:
                    right = jnp.concatenate([left[:, :, half:], right], axis=2)
                    pad = 0
                else:
                    pad = LANES - half
                pieces = [right, jnp.zeros((rows, SUB, half), jnp.float32)]
                if pad:
                    pieces = [jnp.zeros((rows, SUB, pad), jnp.float32)] + pieces
                lower = jnp.concatenate(pieces, axis=2)
            else:
                lower = jnp.zeros_like(upper)
            own = (column >= half) | (column < f * SUB + sub)
            part[:, f * SUB : (f + 1) * SUB, :] = jnp.where(own[None], upper, lower)
        if f == 0:
            pl.semaphore_wait(barrier, len(owners))
        for group in groups:
            if group[-1] == f - 1:
                for i in range(len(owners)):
                    v_copy(i, group).start()
    gathered[walk, member] = part[walk * per + member]
    for group in groups:
        for i in range(len(owners)):
            v_copy(i, group).wait_recv()
    packed_ref[...] = sum(gathered[i] for i in range(1, walks)) + gathered[0]
    for group in groups:
        for i in range(len(owners)):
            v_copy(i, group).wait_send()


def contract(field_rows, cholesky_vectors, per):
    rows, chol = field_rows.shape
    orbitals = cholesky_vectors.shape[1]
    members, walks = lax.axis_size("member"), lax.axis_size("walk")
    half = fold_rows(orbitals)
    vmem = pl.BlockSpec(memory_space=pltpu.VMEM)
    f32, bf16, dma = jnp.float32, jnp.bfloat16, pltpu.SemaphoreType.DMA
    return pl.pallas_call(
        functools.partial(contract_kernel, per),
        in_specs=[vmem, pl.BlockSpec(memory_space=pl.ANY)],
        out_specs=vmem,
        out_shape=jax.ShapeDtypeStruct((members, half, orbitals), f32),
        scratch_shapes=[
            pltpu.VMEM((rows * SUB, chol * SUB), bf16),
            pltpu.VMEM((DEPTH, chol, SUB, LANES), bf16),
            pltpu.VMEM((DEPTH, chol, SUB, orbitals - LANES), bf16),
            pltpu.VMEM((rows, half, orbitals), f32),
            pltpu.VMEM((walks, members, half, orbitals), f32),
            dma((DEPTH,)),
            dma((DEPTH,)),
            dma((walks * members - 1, half // SUB)),
            dma((walks * members - 1, half // SUB)),
        ],
        compiler_params=pltpu.CompilerParams(
            vmem_limit_bytes=48 * 2**20, collective_id=0, has_side_effects=True
        ),
        cost_estimate=pl.CostEstimate(
            flops=2 * rows * SUB * SUB * chol * orbitals * orbitals,
            bytes_accessed=2 * chol * orbitals * orbitals,
            transcendentals=0,
        ),
    )(field_rows, cholesky_vectors)


def eye(size):
    row = lax.broadcasted_iota(jnp.int32, (size, size), 0)
    column = lax.broadcasted_iota(jnp.int32, (size, size), 1)
    return jnp.where(row == column, 1.0, 0.0)


def unfold(packed):
    half, orbitals = packed.shape
    rest = orbitals - half
    row = lax.broadcasted_iota(jnp.int32, (half, half), 0)
    column = lax.broadcasted_iota(jnp.int32, (half, half), 1)
    square = packed[:, :half]
    flipped = -square.T
    first = jnp.where(row > column, square, jnp.where(row < column, flipped, 0.0))
    second = jnp.where(row < column, square, jnp.where(row > column, flipped, 0.0))
    across = packed[:, half:]
    return jnp.concatenate(
        [
            jnp.concatenate([first, across], axis=1),
            jnp.concatenate([-across.T, second[:rest, :rest]], axis=1),
        ],
        axis=0,
    )


def series(v, unit):
    v2 = dot3(v, v)
    v3 = dot3(v2, v)
    upper = unit * (1 / 6) + v * (1 / 24) + v2 * (1 / 120) + v3 * (1 / 720)
    return (unit + v + v2 * 0.5) + dot3(v3, upper)


def chain_kernel(
    packed_ref, trial_ref, deviation_ref, maps_ref, cross_ref, left_ref, walkers_ref,
    steps, held, sent, walk_send, walk_recv, send_sem, recv_sem, w_send, w_recv,
):
    members = packed_ref.shape[0]
    padded, orbitals = held.shape
    electrons = trial_ref.shape[1]
    blocks, block = lax.axis_size("block"), lax.axis_index("block")
    member = lax.axis_index("member")
    has_next, has_last = block < blocks - 1, block > 0
    after, before = lax.rem(block + 1, blocks), lax.rem(block + blocks - 1, blocks)
    bands = padded // SUB
    cuts = [c * bands // CHUNKS * SUB for c in range(CHUNKS)] + [padded]
    others = [lax.rem(member + shift, members) for shift in range(1, members)]
    barrier = greet([{"member": other} for other in others])
    for near, peer in ((has_next, after), (has_last, before)):
        @pl.when(near)
        def _():
            pl.semaphore_signal(barrier, inc=1, device_id={"block": peer}, device_id_type=MESH)

    def w_copy(shift):
        return pltpu.make_async_remote_copy(
            src_ref=walk_send.at[others[shift - 1]],
            dst_ref=walk_recv.at[member],
            send_sem=w_send.at[shift - 1],
            recv_sem=w_recv.at[shift - 1],
            device_id={"member": others[shift - 1]},
            device_id_type=MESH,
        )

    def copy(i):
        at = pl.ds(cuts[i], cuts[i + 1] - cuts[i])
        return pltpu.make_async_remote_copy(
            src_ref=sent.at[at, :],
            dst_ref=held.at[at, :],
            send_sem=send_sem.at[i],
            recv_sem=recv_sem.at[i],
            device_id={"block": before},
            device_id_type=MESH,
        )

    walk_send[...] = trial_ref[...] + deviation_ref[...].astype(jnp.float32)
    unit = eye(orbitals)
    steps[members - 1] = series(unfold(packed_ref[members - 1]), unit)
    pl.semaphore_wait(
        barrier, has_next.astype(jnp.int32) + has_last.astype(jnp.int32) + len(others)
    )
    for shift in range(1, members):
        w_copy(shift).start()
    for s in range(members - 1):
        steps[s] = series(unfold(packed_ref[s]), unit)
    parts = [steps[s] for s in reversed(range(members))]
    while len(parts) > 1:
        paired = [dot3(parts[i], parts[i + 1]) for i in range(0, len(parts) - 1, 2)]
        parts = paired + parts[len(parts) - len(parts) % 2 :]
    maps_ref[0] = parts[0]

    def pass_on(i):
        at = slice(cuts[i], cuts[i + 1])
        sent[at, :] = dot3(held[at, :], maps_ref[0])
        copy(i).start()

    @pl.when(jnp.logical_not(has_next))
    def _():
        held[...] = jnp.zeros_like(held)
        held[:electrons, :] = trial_ref[...].T
        for i in range(CHUNKS):
            pass_on(i)

    maps_ref[members - 1] = steps[members - 1]
    for s in reversed(range(1, members - 1)):
        maps_ref[s] = dot3(maps_ref[s + 1], steps[s])
    @pl.when(has_next & has_last)
    def _():
        for i in range(CHUNKS):
            copy(i).wait_recv()
            pass_on(i)

    walkers_ref[member] = walk_send[member]
    for shift in range(1, members):
        source = lax.rem(member + members - shift, members)
        w_copy(shift).wait()
        walkers_ref[source] = walk_recv[source]
    for s in range(members):
        cross_ref[s] = dot3(maps_ref[s], walkers_ref[s])

    @pl.when(jnp.logical_not(has_last) & has_next)
    def _():
        for i in range(CHUNKS):
            copy(i).wait_recv()

    left_ref[...] = held[:electrons, :]

    @pl.when(has_last)
    def _():
        for i in range(CHUNKS):
            copy(i).wait_send()


def chain(packed, trial_state, deviation):
    members = packed.shape[0]
    orbitals, electrons = trial_state.shape
    padded = -(-electrons // SUB) * SUB
    vmem, dma = pl.BlockSpec(memory_space=pltpu.VMEM), pltpu.SemaphoreType.DMA
    walkers = (members, orbitals, electrons)
    square = (members, orbitals, orbitals)
    return pl.pallas_call(
        chain_kernel,
        in_specs=[vmem] * 3,
        out_specs=[vmem] * 4,
        out_shape=[
            jax.ShapeDtypeStruct(shape, jnp.float32)
            for shape in (square, walkers, (electrons, orbitals), walkers)
        ],
        scratch_shapes=[
            pltpu.VMEM(shape, jnp.float32)
            for shape in (square, (padded, orbitals), (padded, orbitals), walkers, walkers)
        ]
        + [dma((CHUNKS,))] * 2
        + [dma((members - 1,))] * 2,
        compiler_params=pltpu.CompilerParams(
            vmem_limit_bytes=48 * 2**20, collective_id=1, has_side_effects=True
        ),
    )(packed, trial_state, deviation)


def green_kernel(
    scale, left_in_ref, maps_ref, cross_ref, walk_ref, out_ref, left_ref, inter_ref,
    inverse_ref, first_ref,
):
    members = maps_ref.shape[0]
    unit = eye(left_in_ref.shape[0])

    def rounded(a, b):
        return dot_f32(a.astype(jnp.bfloat16), b.astype(jnp.bfloat16))

    levels = []
    for s in range(members):
        inter = dot3(left_in_ref[...], cross_ref[s])
        levels.append(1.0 / jnp.max(jnp.abs(inter), keepdims=True))
        inter_ref[s] = inter * levels[s]
    for s in range(members):
        inter = inter_ref[s]
        flipped = inter.T
        square = rounded(inter, flipped)
        square = rounded(square, square)
        size = jnp.sum(square * square, keepdims=True)
        first = flipped * (START * lax.rsqrt(lax.sqrt(size)))
        inverse_ref[s] = first
        first_ref[s] = first
        left_ref[s] = dot3(left_in_ref[...], maps_ref[s])

    def newton(dot):
        guesses = [inverse_ref[s] for s in range(members)]
        rests = [unit - dot(inter_ref[s], guesses[s]) for s in range(members)]
        for s in range(members):
            inverse_ref[s] = guesses[s] + dot(guesses[s], rests[s])
        return jnp.sum(sum(rest * rest for rest in rests[1:]) + rests[0] * rests[0])

    def rough_round():
        each = range(members)
        guesses = [inverse_ref[s] for s in each]
        powers = [unit - rounded(inter_ref[s], guesses[s]) for s in each]
        for _ in range(2):
            nexts = [rounded(powers[s], powers[s]) for s in each]
            guesses = [guesses[s] + rounded(guesses[s], powers[s]) for s in each]
            powers = nexts
        for s in each:
            inverse_ref[s] = guesses[s] + rounded(guesses[s], powers[s])
        return jnp.sum(sum(power * power for power in powers[1:]) + powers[0] * powers[0])

    def exact(most):
        return lax.while_loop(
            lambda state: (state[0] < most) & (state[1] > REST),
            lambda state: (state[0] + 1, newton(dot3)),
            (jnp.int32(0), jnp.float32(1.0)),
        )[1]

    lax.while_loop(
        lambda state: (state[0] < ROUGH_STEPS) & (state[1] > ROUGH_REST),
        lambda state: (state[0] + 1, rough_round()),
        (jnp.int32(0), jnp.float32(1.0)),
    )
    rest = exact(12)

    @pl.when(jnp.logical_not(rest <= REST))
    def _():
        for s in range(members):
            inverse_ref[s] = first_ref[s]
        exact(80)

    total = None
    for s in range(members):
        solved = dot3(inverse_ref[s], left_ref[s]) * (levels[s] * scale)
        green = dot3(walk_ref[s], solved)
        total = green if total is None else total + green
    out_ref[...] = total


def call(kernel, out_shape, args, scratch=(), scalars=0):
    vmem = pl.BlockSpec(memory_space=pltpu.VMEM)
    smem = pl.BlockSpec(memory_space=pltpu.SMEM)
    return pl.pallas_call(
        kernel,
        in_specs=[smem] * scalars + [vmem] * (len(args) - scalars),
        out_specs=vmem,
        out_shape=out_shape,
        scratch_shapes=list(scratch),
        compiler_params=pltpu.CompilerParams(vmem_limit_bytes=48 * 2**20),
    )(*args)


def spread_kernel(density_ref, out_ref, mine, arrived, whole, *sems):
    sum_send, sum_recv, all_send, all_recv, near_send, near_recv = sems
    orbitals = density_ref.shape[0]
    blocks, piece, _ = mine.shape
    members = whole.shape[0]
    block, member = lax.axis_index("block"), lax.axis_index("member")
    bits = [1 << i for i in reversed(range(members.bit_length() - 1))]
    offsets, pairs = [0], []
    for bit in bits:
        pairs += [(bit, offset) for offset in offsets]
        offsets += [offset + bit for offset in offsets]
    came = {bit + offset: j for j, (bit, offset) in enumerate(pairs)}
    shifts = sorted(range(1, blocks), key=lambda shift: -min(shift, blocks - shift))

    def flip(offset):
        place = member
        for bit in bits:
            if offset & bit:
                place = place + bit - 2 * bit * ((place // bit) % 2)
        return place

    def remote(source, target, send, recv, device):
        return pltpu.make_async_remote_copy(
            src_ref=source, dst_ref=target, send_sem=send, recv_sem=recv,
            device_id=device, device_id_type=MESH,
        )

    def to_sum(shift):
        peer = lax.rem(block + shift, blocks)
        return remote(
            mine.at[peer], arrived.at[shift - 1],
            sum_send.at[shift - 1], sum_recv.at[shift - 1], {"block": peer},
        )

    def to_all(shift):
        ref = whole.at[member, block]
        return remote(
            ref, ref, all_send.at[shift - 1], all_recv.at[shift - 1],
            {"block": lax.rem(block + shift, blocks)},
        )

    def near(j, shift):
        bit, offset = pairs[j]
        ref = whole.at[flip(offset), lax.rem(block + blocks - shift, blocks)]
        return remote(
            ref, ref, near_send.at[j, shift], near_recv.at[j, shift], {"member": flip(bit)}
        )

    barrier = greet(
        [{"block": lax.rem(block + shift, blocks)} for shift in shifts]
        + [{"member": flip(bit)} for bit in bits]
    )
    for q in range(blocks):
        rows = min(piece, orbitals - q * piece)
        if rows > 0:
            mine[q, :rows, :] = density_ref[q * piece : q * piece + rows, :]
        if rows < piece:
            mine[q, max(rows, 0) :, :] = jnp.zeros((piece - max(rows, 0), orbitals), jnp.float32)
    pl.semaphore_wait(barrier, len(shifts) + len(bits))
    for shift in shifts:
        to_sum(shift).start()
    value = mine[block]
    for shift in shifts:
        to_sum(shift).wait_recv()
        value = value + arrived[shift - 1]
    whole[member, block] = value
    for shift in shifts:
        to_all(shift).start()
    for shift in [0] + shifts:
        if shift:
            to_all(shift).wait_recv()
        for j, (bit, offset) in enumerate(pairs):
            if not offset:
                near(j, shift).start()
    waited = set()
    for offset in offsets[1:]:
        for shift in [0] + shifts:
            for j, (bit, held) in enumerate(pairs):
                if held == offset:
                    if (came[offset], shift) not in waited:
                        near(came[offset], shift).wait_recv()
                        waited.add((came[offset], shift))
                    near(j, shift).start()
    for shift in [0] + shifts:
        for j in range(len(pairs)):
            if (j, shift) not in waited:
                near(j, shift).wait_recv()
    for q in range(blocks):
        rows = min(piece, orbitals - q * piece)
        if rows > 0:
            out_ref[:, q * piece : q * piece + rows, :] = whole[:, q, :rows, :]
    for shift in [0] + shifts:
        if shift:
            to_sum(shift).wait_send()
            to_all(shift).wait_send()
        for j in range(len(pairs)):
            near(j, shift).wait_send()


def spread(density):
    blocks, members = lax.axis_size("block"), lax.axis_size("member")
    if members & (members - 1):
        return lax.all_gather(lax.psum(density, "block"), "member")
    orbitals = density.shape[0]
    piece = pl.cdiv(pl.cdiv(orbitals, SUB), blocks) * SUB
    vmem, dma = pl.BlockSpec(memory_space=pltpu.VMEM), pltpu.SemaphoreType.DMA
    return pl.pallas_call(
        spread_kernel,
        in_specs=[vmem],
        out_specs=vmem,
        out_shape=jax.ShapeDtypeStruct((members, orbitals, orbitals), jnp.float32),
        scratch_shapes=[
            pltpu.VMEM((blocks, piece, orbitals), jnp.float32),
            pltpu.VMEM((blocks - 1, piece, orbitals), jnp.float32),
            pltpu.VMEM((members, blocks, piece, orbitals), jnp.float32),
        ]
        + [dma((blocks - 1,))] * 4
        + [dma((members - 1, blocks))] * 2,
        compiler_params=pltpu.CompilerParams(
            vmem_limit_bytes=48 * 2**20, collective_id=2, has_side_effects=True
        ),
    )(density)


def body(fields, cholesky_vectors, trial_state, deviation):
    chol = fields.shape[2]
    orbitals, electrons = trial_state.shape
    blocks, members = lax.axis_size("block"), lax.axis_size("member")
    packed = contract(fields.reshape(-1, chol), cholesky_vectors, deviation.shape[1])
    maps, cross, left, walkers = chain(packed, trial_state, deviation[0])
    square = jax.ShapeDtypeStruct((orbitals, orbitals), jnp.float32)
    density = call(
        functools.partial(green_kernel, 1.0 / (members * blocks)),
        square,
        (left, maps, cross, walkers),
        [pltpu.VMEM((members, electrons, orbitals), jnp.float32)]
        + [pltpu.VMEM((members, electrons, electrons), jnp.float32)] * 3,
    )
    return spread(density)


def solution(mesh):
    sections, walks = mesh.devices.shape

    def run(fields, cholesky_vectors, trial_state, deviation):
        members = deviation.shape[1] // walks
        split_mesh = Mesh(
            mesh.devices.reshape(sections // members, members, walks),
            ("block", "member", "walk"),
        )
        section = ("block", "member")
        in_specs = (
            P(section, None, "walk"),
            P("walk", None, None),
            P(),
            P(section, "walk", None, None),
        )
        return jax.shard_map(
            body, mesh=split_mesh, in_specs=in_specs, out_specs=P("walk", None, None),
            check_vma=False,
        )(fields, cholesky_vectors, trial_state, deviation)

    return run
```
